32 devices in a mesh: dp: 4 (over y, z), tp: 8 (over x, core).
Axes of the slice: x: 4, y: 2, z: 2, core: 2. Of those that a mesh axis runs over, the one named last changes fastest.
The devices are a block of a 4x4x8 slice.
Arguments:
- hidden: bfloat16 [256, 5, 2048], P('dp'), parts along dimension 0
- norm_gain: float32 [2048], replicated
- w_head: bfloat16 [2048, 128256], P(None, 'tp')
- draft_probs: float32 [256, 4, 128256], P('dp', None, 'tp'), parts along dimension 0
- draft_tokens: int32 [256, 4], P('dp'), parts along dimension 0
- temperature: float32 [256], P('dp'), parts along dimension 0
Outputs:
- output 1: float32 [256, 4], P('dp'), parts along dimension 0
- output 2: float32 [256, 4], P('dp'), parts along dimension 0
- output 3: float32 [256, 4, 128256], P('dp', None, 'tp'), parts along dimension 0
- output 4: float32 [256], P('dp'), parts along dimension 0
There are 4 independent parts. The reference program is written for one: setup_inputs(seed, part) draws one part's arguments, and reference() takes and returns one part's arrays. A program takes and returns all parts, laid end to end along the dimension named above; an argument that names none is the same for every part.
All inputs are finite; a program needn't handle non-finite values.
Results may differ from the reference program's by a relative error of at most 0.001.
Values sent between devices are 32-bit elements.
A program may use at most 768 MiB of HBM per device.

```python
import jax
import jax.numpy as jnp
from jax import lax

BATCH_ROWS = 64
DRAFT_LEN = 4
D_MODEL = 2048
VOCAB_SIZE = 128256
CLUSTER_COUNT = 3
WEIGHT_BLOCK = 128
CLUSTER_SPAN = VOCAB_SIZE // 32


def setup_inputs(seed: int = 0, part: int = 0) -> dict:
    part_key = jax.random.fold_in(jax.random.key(seed), part)
    key_h, key_q, key_s, key_t, key_c, key_k, key_o = jax.random.split(part_key, 7)
    key_w, key_g = jax.random.split(jax.random.key(seed + 1), 2)
    hidden = jax.random.normal(key_h, (BATCH_ROWS, DRAFT_LEN + 1, D_MODEL), jnp.float32).astype(jnp.bfloat16)
    norm_gain = jax.random.uniform(key_g, (D_MODEL,), jnp.float32, 0.5, 1.5)

    def weight_block(block_idx):
        gauss_block = jax.random.normal(jax.random.fold_in(key_w, block_idx), (WEIGHT_BLOCK, VOCAB_SIZE), jnp.float32)
        return (gauss_block * D_MODEL ** -0.5).astype(jnp.bfloat16)

    w_head = lax.map(weight_block, jnp.arange(D_MODEL // WEIGHT_BLOCK)).reshape(D_MODEL, VOCAB_SIZE)
    q_scale = jax.random.uniform(key_s, (BATCH_ROWS, DRAFT_LEN, 1), jnp.float32, 0.7, 1.3)
    q_logits = jax.random.normal(key_q, (BATCH_ROWS, DRAFT_LEN, VOCAB_SIZE), jnp.float32) * q_scale
    draft_probs = jax.nn.softmax(q_logits, axis=-1)
    temperature = jax.random.uniform(key_t, (BATCH_ROWS,), jnp.float32, 0.6, 1.4)
    centers = jax.random.randint(key_c, (CLUSTER_COUNT,), 0, VOCAB_SIZE - CLUSTER_SPAN)
    choice = jax.random.randint(key_k, (BATCH_ROWS, DRAFT_LEN), 0, CLUSTER_COUNT)
    offsets = jax.random.randint(key_o, (BATCH_ROWS, DRAFT_LEN), 0, CLUSTER_SPAN)
    draft_tokens = (centers[choice] + offsets).astype(jnp.int32)
    return {'hidden': hidden, 'norm_gain': norm_gain, 'w_head': w_head, 'draft_probs': draft_probs, 'draft_tokens': draft_tokens, 'temperature': temperature}


def reference(hidden, norm_gain, w_head, draft_probs, draft_tokens, temperature):
    def one_row(row_args):
        row_hidden, row_probs, row_tokens, row_temp = row_args
        hidden_f32 = row_hidden.astype(jnp.float32)
        inv_rms = lax.rsqrt(jnp.mean(hidden_f32 * hidden_f32, axis=-1, keepdims=True) + 1e-5)
        normed = (hidden_f32 * inv_rms * norm_gain).astype(jnp.bfloat16)
        logits = jnp.dot(normed, w_head, preferred_element_type=jnp.float32)
        scaled = logits / row_temp
        row_max = jnp.max(scaled, axis=-1, keepdims=True)
        row_lse = row_max + jnp.log(jnp.sum(jnp.exp(scaled - row_max), axis=-1, keepdims=True))
        target = jnp.exp(scaled[:DRAFT_LEN] - row_lse[:DRAFT_LEN])
        tok_target = jnp.take_along_axis(target, row_tokens[:, None], axis=-1)[:, 0]
        tok_draft = jnp.take_along_axis(row_probs, row_tokens[:, None], axis=-1)[:, 0]
        accept = jnp.minimum(1.0, tok_target / tok_draft)
        excess = jnp.maximum(target - row_probs, 0.0)
        norm_sum = jnp.sum(excess, axis=-1)
        residual = excess / norm_sum[:, None]
        return accept, norm_sum, residual, row_lse[DRAFT_LEN, 0]

    accept, norm_sum, residual, bonus_lse = lax.map(one_row, (hidden, draft_probs, draft_tokens, temperature))
    return accept, norm_sum, residual, bonus_lse
```

```python
import functools

import jax
import jax.numpy as jnp
from jax import lax
from jax.experimental import pallas as pl
from jax.experimental.pallas import tpu as pltpu
from jax.sharding import PartitionSpec as P

LANES = 128
TILE = 256
STEP = 2 * TILE
RING = 8
GRANT = 24 * 1024 * 1024
LOG2E = 1.4426950408889634
LN2 = 0.6931471805599453
LOWEST = -3.4028234e38
MESH = pl.DeviceIdType.MESH


def _row_to_col(row):
    n = row.shape[1]
    r = lax.broadcasted_iota(jnp.int32, (n, n), 0)
    c = lax.broadcasted_iota(jnp.int32, (n, n), 1)
    return jnp.sum(jnp.where(r == c, row, 0.0), axis=1, keepdims=True)


def _col_to_row(col):
    n = col.shape[0]
    r = lax.broadcasted_iota(jnp.int32, (n, n), 0)
    c = lax.broadcasted_iota(jnp.int32, (n, n), 1)
    return jnp.sum(jnp.where(r == c, col, 0.0), axis=0, keepdims=True)


def _logits_kernel(
    dims,
    x_hbm, gain_ref, w_hbm, q_hbm, temp_ref,
    s_ref, q_buf, msg1,
    h_buf, x_buf, w_buf, q_last, m_buf, l_buf, scale_buf,
    h_sem, w_sem, q_sem,
):
    batch, draft, depth, vocab = dims
    rows = batch * (draft + 1)
    nk = depth // TILE
    full = vocab // STEP
    rest = vocab - full * STEP
    nc = -(-vocab // LANES)
    last = vocab - (nc - 1) * LANES
    def w_copy(n, size=STEP):
        slot = lax.rem(n, RING)
        return pltpu.make_async_copy(
            w_hbm.at[pl.ds(n * STEP, size), :], w_buf.at[slot, pl.ds(0, size), :], w_sem.at[slot])

    qv = q_buf.reshape(nc, batch, draft, LANES)

    def q_copy(c):
        return pltpu.make_async_copy(
            q_hbm.at[:, :, pl.ds(pl.multiple_of(c * LANES, LANES), LANES)], qv.at[c], q_sem.at[c])

    def last_q():
        return pltpu.make_async_copy(
            q_hbm.at[:, :, pl.ds((nc - 1) * LANES, last)], q_last, q_sem.at[nc - 1])

    h_copy = pltpu.make_async_copy(x_hbm, h_buf, h_sem)
    h_copy.start()
    for n in range(RING - 1):
        w_copy(n).start()

    temp_col = _row_to_col(temp_ref[...])
    scale_buf[...] = jnp.broadcast_to(LOG2E / temp_col, (batch, LANES))
    m_buf[...] = jnp.full_like(m_buf, LOWEST)
    l_buf[...] = jnp.zeros_like(l_buf)

    h_copy.wait()

    @pl.loop(0, rows // 16)
    def _(i):
        sl = pl.ds(pl.multiple_of(i * 16, 16), 16)
        h = h_buf[sl, :].astype(jnp.float32)
        r = lax.rsqrt(jnp.mean(h * h, axis=-1, keepdims=True) + 1e-5)
        x_buf[sl, :] = (h * r * gain_ref[...]).astype(jnp.bfloat16)

    groups = draft + 1

    def online(g, q, c0, z, ncol, penalty=None):
        rs = pl.ds(g * batch, batch)
        scale = scale_buf[...]
        ss = [z[:, i * LANES:(i + 1) * LANES] * scale for i in range(ncol)]
        if penalty is not None:
            ss = [s + p for s, p in zip(ss, penalty)]
        m_old = m_buf[rs, :]
        m_new = m_old
        for s in ss:
            m_new = jnp.maximum(m_new, s)
        l = l_buf[rs, :] * jnp.exp2(m_old - m_new)
        for s in ss:
            l = l + jnp.exp2(s - m_new)
        m_buf[rs, :] = m_new
        l_buf[rs, :] = l
        if g < draft:
            for i in range(ncol):
                s_ref[c0 + i, pl.ds(g, batch, stride=draft), :] = ss[i]

    def lhs(g, k):
        return x_buf[pl.ds(g * batch, batch), pl.ds(k * TILE, TILE)]

    def push(n, q, k):
        slot = lax.rem(n, RING)
        w = w_buf[slot, pl.ds(q * TILE, TILE), pl.ds(k * TILE, TILE)]
        pltpu.matmul_push_rhs(w, staging_register=k % 2, mxu_index=q, transpose=True)

    def mxu_body(*accs):
        acc = [[[accs[(a * 2 + q) * groups + g] for g in range(groups)] for q in range(2)] for a in range(2)]
        for a in range(2):
            for q in range(2):
                for g in range(groups):
                    pltpu.matmul_pop(acc[a][q][g])

        def fullstep(n, a, issue, penalty=None, next_full=True):
            old = acc[1 - a]
            c_old = jnp.maximum(n - 1, 0) * (STEP // LANES)
            for k in range(nk):
                for q in range(2):
                    for g in range(groups):
                        pltpu.matmul_acc_lhs(acc[a][q][g], lhs(g, k), load_staged_rhs=k % 2 if g == 0 else None)
                for q in range(2):
                    if k + 1 < nk:
                        push(n, q, k + 1)
                    elif next_full:
                        push(n + 1, q, 0)
                if k == 1:
                    issue()
                if 1 <= k <= groups:
                    g = k - 1
                    for q in range(2):
                        z = pltpu.matmul_pop(old[q][g])
                        online(g, q, c_old + q * (TILE // LANES), z, TILE // LANES,
                               None if penalty is None else [penalty] * (TILE // LANES))

        w_copy(0).wait()
        for q in range(2):
            push(0, q, 0)

        split = (full - (RING - 1)) // 2 * 2
        tail = full // 2 * 2
        early = 2
        per = 8
        mid = nc - 1 - early * split - per * (tail - split)

        def issue_early(n):
            w_copy(n + RING - 1).start()
            for i in range(early):
                q_copy(n * early + i).start()

        def issue_late(n):
            for i in range(per):
                q_copy(early * split + mid + (n - split) * per + i).start()

        @pl.loop(0, split // 2)
        def _(i):
            n = 2 * i
            w_copy(n + 1).wait()
            fullstep(n, 0, lambda: issue_early(n), penalty=jnp.where(i == 0, LOWEST, 0.0).astype(jnp.float32))
            w_copy(n + 2).wait()
            fullstep(n + 1, 1, lambda: issue_early(n + 1))

        w_copy(full, rest).start()

        last_q().start()

        @pl.loop(0, mid)
        def _(i):
            q_copy(early * split + i).start()

        @pl.loop(split // 2, tail // 2)
        def _(i):
            n = 2 * i
            w_copy(n + 1).wait()
            fullstep(n, 0, lambda: issue_late(n))
            w_copy(n + 2).wait()
            fullstep(n + 1, 1, lambda: issue_late(n + 1))

        assert tail == full - 1
        n = full - 1
        w_copy(full, rest).wait()
        fullstep(n, 0, lambda: None, next_full=False)
        slot = full % RING
        half = nk // 2
        for kk in range(half):
            for q in range(2):
                k = q * half + kk
                w = w_buf[slot, pl.ds(0, TILE), pl.ds(k * TILE, TILE)]
                pltpu.matmul_push_rhs(w, staging_register=kk % 2, mxu_index=q, transpose=True)
                for g in range(groups):
                    pltpu.matmul_acc_lhs(acc[1][q][g], lhs(g, k), load_staged_rhs=kk % 2 if g == 0 else None)
        for g in range(groups):
            for q in range(2):
                z = pltpu.matmul_pop(acc[0][q][g])
                online(g, q, n * (STEP // LANES) + q * (TILE // LANES), z, TILE // LANES)
        ncol = -(-rest // LANES)
        lane = lax.broadcasted_iota(jnp.int32, (batch, LANES), 1)
        pens = [None] * ncol
        for i in range(ncol):
            pens[i] = jnp.where(lane + i * LANES < rest, 0.0, LOWEST)
        for g in range(groups):
            z = pltpu.matmul_pop(acc[1][0][g]) + pltpu.matmul_pop(acc[1][1][g])
            online(g, 0, full * (STEP // LANES), z, ncol, pens)

    specs = [pltpu.ACC(q)((batch, TILE), jnp.float32) for a in range(2) for q in range(2) for g in range(groups)]
    pl.run_scoped(mxu_body, *specs)

    msg1[...] = jnp.zeros_like(msg1)
    for g in range(groups):
        rs = pl.ds(g * batch, batch)
        m = m_buf[rs, :]
        top = jnp.max(m, axis=1, keepdims=True)
        tot = jnp.sum(l_buf[rs, :] * jnp.exp2(m - top), axis=1, keepdims=True)
        msg1[pl.ds(g, 1), pl.ds(0, batch)] = _col_to_row(top + jnp.log2(tot))

    @pl.loop(0, nc - 1)
    def _(c):
        q_copy(c).wait()

    last_q().wait()
    for b in range(0, batch, 2):
        q_buf[nc - 1, pl.ds(b * draft, 2 * draft), pl.ds(0, last)] = jnp.concatenate([q_last[b], q_last[b + 1]], axis=0)


def _verify_kernel(
    dims,
    s_ref, q_ref, msg1, tok_smem, tok_ref,
    col_buf, inv_ref, accept_ref, norm_ref, bonus_ref,
    gs_buf, gq_buf, part_buf,
    msg2, got1, got2,
    send1, recv1, send2, recv2,
):
    batch, draft, vocab, ntp = dims
    nc = -(-vocab // LANES)
    last = vocab - (nc - 1) * LANES
    me = lax.axis_index("tp")
    barrier = pltpu.get_barrier_semaphore()
    for d in range(1, ntp):
        pl.semaphore_signal(barrier, inc=1, device_id={"tp": lax.rem(me + d, ntp)}, device_id_type=MESH)
    pl.semaphore_wait(barrier, ntp - 1)

    def remote(msg, got, send, recv, d):
        return pltpu.make_async_remote_copy(
            src_ref=msg, dst_ref=got.at[me], send_sem=send.at[d], recv_sem=recv.at[me],
            device_id={"tp": lax.rem(me + d, ntp)}, device_id_type=MESH)

    def arrived(msg, got, send, recv, d):
        src = lax.rem(me + d, ntp)
        return pltpu.make_async_remote_copy(
            src_ref=msg, dst_ref=got.at[src], send_sem=send.at[d], recv_sem=recv.at[src],
            device_id={"tp": src}, device_id_type=MESH)

    for d in range(1, ntp):
        remote(msg1, got1, send1, recv1, d).start()
    got1[me] = msg1[...]

    @pl.loop(0, batch)
    def _(b):
        for j in range(draft):
            idx = tok_smem[j, b] - me * vocab
            idx = jnp.minimum(jnp.maximum(idx, 0), vocab - 1)
            c = lax.shift_right_logical(idx, 7)
            gs_buf[pl.ds(j * batch + b, 1), :] = s_ref[c, pl.ds(b * draft + j, 1), :]
            gq_buf[pl.ds(j * batch + b, 1), :] = q_ref[c, pl.ds(b * draft + j, 1), :]

    msg2[...] = jnp.zeros_like(msg2)
    lane = lax.broadcasted_iota(jnp.int32, (batch, LANES), 1)
    for j in range(draft):
        idx = _row_to_col(tok_ref[pl.ds(j, 1), :].astype(jnp.float32)).astype(jnp.int32) - me * vocab
        owned = jnp.logical_and(idx >= 0, idx < vocab)
        hit = jnp.logical_and(owned, lane == jnp.bitwise_and(idx, LANES - 1))
        rs = pl.ds(j * batch, batch)
        tok_s = jnp.sum(jnp.where(hit, gs_buf[rs, :], 0.0), axis=1, keepdims=True)
        tok_q = jnp.sum(jnp.where(hit, gq_buf[rs, :], 0.0), axis=1, keepdims=True)
        msg2[pl.ds(draft + j, 1), pl.ds(0, batch)] = _col_to_row(tok_s)
        msg2[pl.ds(2 * draft + j, 1), pl.ds(0, batch)] = _col_to_row(tok_q)

    for d in range(1, ntp):
        arrived(msg1, got1, send1, recv1, d).wait_recv()
    top = got1[0]
    for i in range(1, ntp):
        top = jnp.maximum(top, got1[i])
    tot = jnp.exp2(got1[0] - top)
    for i in range(1, ntp):
        tot = tot + jnp.exp2(got1[i] - top)
    lse2 = top + jnp.log2(tot)
    bonus_ref[...] = lse2[draft:draft + 1, 0:batch] * LN2
    for j in range(draft):
        col_buf[pl.ds(j, batch, stride=draft), :] = jnp.broadcast_to(
            _row_to_col(lse2[j:j + 1, 0:batch]), (batch, LANES))

    nv = batch * draft // 8
    unroll = 25 if (nc - 1) % 25 == 0 else 1
    last_mask = lax.broadcasted_iota(jnp.int32, (8, LANES), 1) < last

    @pl.loop(0, nv // 2)
    def _(v):
        rss = [pl.ds(pl.multiple_of((2 * v + i) * 8, 8), 8) for i in range(2)]
        ls = [col_buf[rs, :] for rs in rss]

        def ex(c, i):
            return jnp.maximum(jnp.exp2(s_ref[c, rss[i], :] - ls[i]) - q_ref[c, rss[i], :], 0.0)

        def inner(t, sums):
            sums = list(sums)
            for u in range(unroll):
                c = t * unroll + u
                for i in range(2):
                    sums[i] = sums[i] + ex(c, i)
            return tuple(sums)

        zero = jnp.zeros((8, LANES), jnp.float32)
        sums = lax.fori_loop(0, (nc - 1) // unroll, inner, (zero, zero))
        for i in range(2):
            e = jnp.where(last_mask, ex(nc - 1, i), 0.0)
            part_buf[rss[i], :] = sums[i] + e

    for j in range(draft):
        part = jnp.sum(part_buf[pl.ds(j, batch, stride=draft), :], axis=1, keepdims=True)
        msg2[pl.ds(j, 1), pl.ds(0, batch)] = _col_to_row(part)

    for d in range(1, ntp):
        remote(msg2, got2, send2, recv2, d).start()
    got2[me] = msg2[...]
    for d in range(1, ntp):
        arrived(msg2, got2, send2, recv2, d).wait_recv()
    tot = got2[0]
    for i in range(1, ntp):
        tot = tot + got2[i]
    norm = tot[0:draft, 0:batch]
    norm_ref[...] = norm
    target = jnp.exp2(tot[draft:2 * draft, 0:batch] - lse2[0:draft, 0:batch])
    accept_ref[...] = jnp.minimum(1.0, target / tot[2 * draft:3 * draft, 0:batch])
    for j in range(draft):
        inv_ref[pl.ds(j, batch, stride=draft), :] = jnp.broadcast_to(
            1.0 / _row_to_col(norm[j:j + 1, :]), (batch, LANES))
    for d in range(1, ntp):
        remote(msg1, got1, send1, recv1, d).wait_send()
        remote(msg2, got2, send2, recv2, d).wait_send()


OUT_RING = 4
OUT_GROUP = 5


def _write_kernel(
    dims, s_ref, q_ref, lse_ref, inv_ref, accept_in, norm_in, bonus_in,
    out_hbm, accept_ref, norm_ref, bonus_ref, stage, stage_last, sem,
):
    batch, draft, vocab = dims
    accept_ref[...] = accept_in[...]
    norm_ref[...] = norm_in[...]
    bonus_ref[...] = bonus_in[...]
    nc = -(-vocab // LANES)
    view = stage.reshape(OUT_RING * OUT_GROUP, batch, draft, LANES)
    ngroups = (nc - 1) // OUT_GROUP
    assert ngroups * OUT_GROUP == nc - 1

    def copy(slot, c):
        return pltpu.make_async_copy(
            view.at[slot], out_hbm.at[:, :, pl.ds(pl.multiple_of(c * LANES, LANES), LANES)], sem.at[slot])

    def fill(slot, c):
        stage[slot] = jnp.maximum(jnp.exp2(s_ref[c] - lse_ref[...]) - q_ref[c], 0.0) * inv_ref[...]

    @pl.loop(0, ngroups)
    def _(t):
        base = lax.rem(t, OUT_RING) * OUT_GROUP

        @pl.when(t >= OUT_RING)
        def _():
            for i in range(OUT_GROUP):
                copy(base + i, (t - OUT_RING) * OUT_GROUP + i).wait()

        for i in range(OUT_GROUP):
            fill(base + i, t * OUT_GROUP + i)
            copy(base + i, t * OUT_GROUP + i).start()

    for t in range(ngroups - OUT_RING, ngroups):
        for i in range(OUT_GROUP):
            copy(t % OUT_RING * OUT_GROUP + i, t * OUT_GROUP + i).wait()
    c = nc - 1
    last = vocab - c * LANES
    fill(0, c)
    for b in range(batch):
        rs = pl.ds(b * draft, draft)
        stage_last[b] = stage[0, rs, pl.ds(0, last)]
    final = pltpu.make_async_copy(stage_last, out_hbm.at[:, :, pl.ds(c * LANES, last)], sem.at[0])
    final.start()
    final.wait()


def solution(mesh):
    ntp = mesh.shape["tp"]

    def local_step(hidden, norm_gain, w_head, draft_probs, draft_tokens, temperature):
        batch, draft, vocab = draft_probs.shape
        depth = hidden.shape[2]
        rows = batch * (draft + 1)
        nc = -(-vocab // LANES)
        vmem = pl.BlockSpec(memory_space=pltpu.VMEM)
        hbm = pl.BlockSpec(memory_space=pl.ANY)
        smem = pl.BlockSpec(memory_space=pltpu.SMEM)
        keep = functools.partial(pltpu.with_memory_space_constraint, memory_space=pltpu.VMEM)
        f32, bf16, dma = jnp.float32, jnp.bfloat16, pltpu.SemaphoreType.DMA
        vec = pltpu.VMEM((batch * draft, LANES), f32)
        big = pltpu.VMEM((nc, batch * draft, LANES), f32)
        x = hidden.transpose(1, 0, 2).reshape(rows, depth)
        tok = draft_tokens.T
        s, q, lse = pl.pallas_call(
            functools.partial(_logits_kernel, (batch, draft, depth, vocab)),
            out_shape=(big, big, pltpu.VMEM((8, LANES), f32)),
            in_specs=[hbm, vmem, hbm, hbm, vmem],
            out_specs=(vmem,) * 3,
            scratch_shapes=[
                pltpu.VMEM((rows, depth), bf16),
                pltpu.VMEM((rows, depth), bf16),
                pltpu.VMEM((RING, STEP, depth), bf16),
                pltpu.VMEM((batch, draft, vocab - (nc - 1) * LANES), f32),
                pltpu.VMEM((rows, LANES), f32),
                pltpu.VMEM((rows, LANES), f32),
                pltpu.VMEM((batch, LANES), f32),
                dma,
                dma((RING,)),
                dma((nc,)),
            ],
            compiler_params=pltpu.CompilerParams(vmem_limit_bytes=GRANT),
            name="logits",
        )(x, norm_gain.reshape(1, depth), w_head.T, draft_probs, temperature.reshape(1, batch))
        lse, inv, accept, norm, bonus = pl.pallas_call(
            functools.partial(_verify_kernel, (batch, draft, vocab, ntp)),
            out_shape=(
                vec,
                vec,
                pltpu.VMEM((draft, batch), f32),
                pltpu.VMEM((draft, batch), f32),
                pltpu.VMEM((1, batch), f32),
            ),
            in_specs=[vmem, vmem, vmem, smem, vmem],
            out_specs=(vmem,) * 5,
            scratch_shapes=[
                vec, vec, vec,
                pltpu.VMEM((16, LANES), f32),
                pltpu.VMEM((ntp, 8, LANES), f32),
                pltpu.VMEM((ntp, 16, LANES), f32),
                dma((ntp,)), dma((ntp,)), dma((ntp,)), dma((ntp,)),
            ],
            compiler_params=pltpu.CompilerParams(
                collective_id=0, has_side_effects=True, vmem_limit_bytes=GRANT),
            name="verify",
        )(keep(s), keep(q), keep(lse), tok, tok)
        residual, accept, norm, bonus = pl.pallas_call(
            functools.partial(_write_kernel, (batch, draft, vocab)),
            out_shape=(
                jax.ShapeDtypeStruct(draft_probs.shape, f32),
                jax.ShapeDtypeStruct((draft, batch), f32),
                jax.ShapeDtypeStruct((draft, batch), f32),
                jax.ShapeDtypeStruct((1, batch), f32),
            ),
            in_specs=[vmem] * 7,
            out_specs=(hbm, vmem, vmem, vmem),
            scratch_shapes=[
                pltpu.VMEM((OUT_RING * OUT_GROUP, batch * draft, LANES), f32),
                pltpu.VMEM((batch, draft, vocab - (nc - 1) * LANES), f32),
                dma((OUT_RING * OUT_GROUP,)),
            ],
            compiler_params=pltpu.CompilerParams(vmem_limit_bytes=GRANT),
            name="write",
        )(*map(keep, (s, q, lse, inv, accept, norm, bonus)))
        return accept.T, norm.T, residual, bonus.reshape(batch)

    return jax.shard_map(
        local_step,
        mesh=mesh,
        in_specs=(P('dp', None, None), P(), P(None, 'tp'), P('dp', None, 'tp'), P('dp', None), P('dp')),
        out_specs=(P('dp', None), P('dp', None), P('dp', None, 'tp'), P('dp')),
        check_vma=False,
    )
```

```python
import functools

import jax
import jax.numpy as jnp
from jax import lax
from jax.experimental import pallas as pl
from jax.experimental.pallas import tpu as pltpu
from jax.sharding import PartitionSpec as P

LANES = 128
TILE = 256
STEP = 2 * TILE
RING = 8
W_PARTS = 4
FENCES = 6
SIG = (1, 3, 5, 7)
GRP = {1: (0,), 3: (1, 2), 5: (3, 4)}
GRANT = 24 * 1024 * 1024
LOG2E = 1.4426950408889634
LN2 = 0.6931471805599453
LOWEST = -3.4028234e38
MESH = pl.DeviceIdType.MESH


def _row_to_col(row):
    n = row.shape[1]
    r = lax.broadcasted_iota(jnp.int32, (n, n), 0)
    c = lax.broadcasted_iota(jnp.int32, (n, n), 1)
    return jnp.sum(jnp.where(r == c, row, 0.0), axis=1, keepdims=True)


def _col_to_row(col):
    n = col.shape[0]
    r = lax.broadcasted_iota(jnp.int32, (n, n), 0)
    c = lax.broadcasted_iota(jnp.int32, (n, n), 1)
    return jnp.sum(jnp.where(r == c, col, 0.0), axis=0, keepdims=True)


def _logits_kernel(
    dims,
    x_hbm, gain_ref, w_hbm, q_hbm, temp_ref,
    s_ref, q_buf, m_buf, l_buf,
    h_buf, x_buf, w_buf, q_last, scale_buf,
    h_sem, w_sem, q_sem, fence,
):
    batch, draft, depth, vocab = dims
    rows = batch * (draft + 1)
    nk = depth // TILE
    full = vocab // STEP
    rest = vocab - full * STEP
    nc = -(-vocab // LANES)
    last = vocab - (nc - 1) * LANES
    part = STEP // W_PARTS

    def w_copy(n, i, size=part):
        slot = lax.rem(n, RING)
        return pltpu.make_async_copy(
            w_hbm.at[pl.ds(n * STEP + i * part, size), :], w_buf.at[slot, pl.ds(i * part, size), :], w_sem.at[slot, i])

    def w_wait(n):
        for i in range(W_PARTS):
            w_copy(n, i).wait()

    def w_rest():
        return [w_copy(full, i, min(part, rest - i * part)) for i in range(-(-rest // part))]

    qv = q_buf.reshape(nc, batch, draft, LANES)

    def q_copy(c):
        return pltpu.make_async_copy(
            q_hbm.at[:, :, pl.ds(pl.multiple_of(c * LANES, LANES), LANES)], qv.at[c], q_sem.at[0])

    def last_q():
        return pltpu.make_async_copy(
            q_hbm.at[:, :, pl.ds((nc - 1) * LANES, last)], q_last, q_sem.at[1])

    h_copy = pltpu.make_async_copy(x_hbm, h_buf, h_sem)
    h_copy.start()
    for n in range(RING - 1):
        for i in range(W_PARTS):
            w_copy(n, i).start()
    last_q().start(priority=1)

    temp_col = _row_to_col(temp_ref[...])
    scale_buf[...] = jnp.broadcast_to(LOG2E / temp_col, (batch, LANES))
    m_buf[...] = jnp.full_like(m_buf, LOWEST)
    l_buf[...] = jnp.zeros_like(l_buf)

    groups = draft + 1

    def online(g, q, c0, z, ncol, penalty=None):
        rs = pl.ds(g * batch, batch)
        scale = scale_buf[...]
        ss = [z[:, i * LANES:(i + 1) * LANES] * scale for i in range(ncol)]
        if penalty is not None:
            ss = [s + p for s, p in zip(ss, penalty)]
        m_old = m_buf[rs, :]
        m_new = m_old
        for s in ss:
            m_new = jnp.maximum(m_new, s)
        l = l_buf[rs, :] * jnp.exp2(m_old - m_new)
        for s in ss:
            l = l + jnp.exp2(s - m_new)
        m_buf[rs, :] = m_new
        l_buf[rs, :] = l
        if g < draft:
            for i in range(ncol):
                s_ref[c0 + i, pl.ds(g, batch, stride=draft), :] = ss[i]

    def lhs(g, k):
        return x_buf[pl.ds(g * batch, batch), pl.ds(k * TILE, TILE)]

    def push(n, q, k):
        slot = lax.rem(n, RING)
        w = w_buf[slot, pl.ds(q * TILE, TILE), pl.ds(k * TILE, TILE)]
        pltpu.matmul_push_rhs(w, staging_register=k % 2, mxu_index=q, transpose=True)

    def mxu_body(*accs):
        acc = [[[accs[(a * 2 + q) * groups + g] for g in range(groups)] for q in range(2)] for a in range(2)]
        for a in range(2):
            for q in range(2):
                for g in range(groups):
                    pltpu.matmul_pop(acc[a][q][g])

        h_copy.wait()
        for i in range(rows // 32):
            sl = pl.ds(i * 32, 32)
            h = h_buf[sl, :].astype(jnp.float32)
            r = lax.rsqrt(jnp.mean(h * h, axis=-1, keepdims=True) + 1e-5)
            x_buf[sl, :] = (h_buf[sl, :].astype(jnp.float32) * r * gain_ref[...]).astype(jnp.bfloat16)

        half = nk // 2

        def push_rest(q, kk):
            w = w_buf[full % RING, pl.ds(0, TILE), pl.ds((q * half + kk) * TILE, TILE)]
            pltpu.matmul_push_rhs(w, staging_register=kk % 2, mxu_index=q, transpose=True)

        def fullstep(n, a, issue, penalty=None, next_full=True):
            old = acc[1 - a]
            c_old = jnp.maximum(n - 1, 0) * (STEP // LANES)
            for k in range(nk):
                for q in range(2):
                    for g in range(groups):
                        pltpu.matmul_acc_lhs(acc[a][q][g], lhs(g, k), load_staged_rhs=k % 2 if g == 0 else None)
                for q in range(2):
                    if k + 1 < nk:
                        push(n, q, k + 1)
                    elif next_full:
                        push(n + 1, q, 0)
                    else:
                        push_rest(q, 0)
                if 1 <= k <= FENCES:
                    issue(k - 1)
                if k in SIG:
                    pl.semaphore_signal(fence, 1)
                for g in GRP.get(k, ()):
                    for q in range(2):
                        z = pltpu.matmul_pop(old[q][g])
                        online(g, q, c_old + q * (TILE // LANES), z, TILE // LANES,
                               None if penalty is None else [penalty] * (TILE // LANES))

            pl.semaphore_wait(fence, len(SIG))

        w_wait(0)
        for q in range(2):
            push(0, q, 0)

        split = (full - (RING - 1)) // 2 * 2
        tail = full // 2 * 2
        early = FENCES - W_PARTS
        late = 8
        final = FENCES
        mid = nc - 1 - early * split - late * (tail - split) - final
        assert mid >= 0 and tail == full - 1

        def issue_early(n, i):
            if i < W_PARTS:
                w_copy(n + RING - 1, i).start()
            else:
                q_copy(n * early + i - W_PARTS).start(priority=1)

        def issue_late(n, i):
            base = early * split + mid + (n - split) * late
            q_copy(base + i).start(priority=1)
            if i < late - FENCES:
                q_copy(base + FENCES + i).start(priority=1)

        def issue_final(i):
            q_copy(nc - 1 - final + i).start(priority=1)

        @pl.loop(0, split // 2)
        def _(t):
            n = 2 * t
            w_wait(n + 1)
            fullstep(n, 0, lambda i: issue_early(n, i), penalty=jnp.where(t == 0, LOWEST, 0.0).astype(jnp.float32))
            w_wait(n + 2)
            fullstep(n + 1, 1, lambda i: issue_early(n + 1, i))

        for copy in w_rest():
            copy.start()

        @pl.loop(0, mid)
        def _(i):
            q_copy(early * split + i).start(priority=1)

        @pl.loop(split // 2, tail // 2)
        def _(t):
            n = 2 * t
            w_wait(n + 1)
            fullstep(n, 0, lambda i: issue_late(n, i))
            w_wait(n + 2)
            fullstep(n + 1, 1, lambda i: issue_late(n + 1, i))

        n = full - 1
        for copy in w_rest():
            copy.wait()
        last_q().wait()
        for b in range(0, batch, 2):
            q_buf[nc - 1, pl.ds(b * draft, 2 * draft), pl.ds(0, last)] = jnp.concatenate([q_last[b], q_last[b + 1]], axis=0)
        fullstep(n, 0, issue_final, next_full=False)
        for kk in range(half):
            for q in range(2):
                for g in range(groups):
                    pltpu.matmul_acc_lhs(acc[1][q][g], lhs(g, q * half + kk), load_staged_rhs=kk % 2 if g == 0 else None)
                if kk + 1 < half:
                    push_rest(q, kk + 1)
        for g in range(groups):
            for q in range(2):
                z = pltpu.matmul_pop(acc[0][q][g])
                online(g, q, n * (STEP // LANES) + q * (TILE // LANES), z, TILE // LANES)
        ncol = -(-rest // LANES)
        lane = lax.broadcasted_iota(jnp.int32, (batch, LANES), 1)
        pens = [None] * ncol
        for i in range(ncol):
            pens[i] = jnp.where(lane + i * LANES < rest, 0.0, LOWEST)
        for g in range(groups):
            z = pltpu.matmul_pop(acc[1][0][g]) + pltpu.matmul_pop(acc[1][1][g])
            online(g, 0, full * (STEP // LANES), z, ncol, pens)

    specs = [pltpu.ACC(q)((batch, TILE), jnp.float32) for a in range(2) for q in range(2) for g in range(groups)]
    pl.run_scoped(mxu_body, *specs)

    bulk = q_buf.at[pl.ds(0, nc - 1)]
    pltpu.make_async_copy(bulk, bulk, q_sem.at[0]).wait()


def _verify_kernel(
    dims,
    s_ref, q_ref, m_ref, l_ref, tok_smem, tok_ref,
    col_buf, inv_ref, accept_ref, norm_ref, bonus_ref,
    gs_buf, gq_buf, part_buf,
    msg1, msg2, got1, got2,
    send1, recv1, send2, recv2,
):
    batch, draft, vocab, ntp = dims
    nc = -(-vocab // LANES)
    last = vocab - (nc - 1) * LANES
    me = lax.axis_index("tp")
    barrier = pltpu.get_barrier_semaphore()
    for d in range(1, ntp):
        pl.semaphore_signal(barrier, inc=1, device_id={"tp": lax.rem(me + d, ntp)}, device_id_type=MESH)

    def remote(msg, got, send, recv, d):
        return pltpu.make_async_remote_copy(
            src_ref=msg, dst_ref=got.at[me], send_sem=send.at[d], recv_sem=recv.at[me],
            device_id={"tp": lax.rem(me + d, ntp)}, device_id_type=MESH)

    def arrived(msg, got, send, recv, d):
        src = lax.rem(me + d, ntp)
        return pltpu.make_async_remote_copy(
            src_ref=msg, dst_ref=got.at[src], send_sem=send.at[d], recv_sem=recv.at[src],
            device_id={"tp": src}, device_id_type=MESH)

    msg1[...] = jnp.zeros_like(msg1)
    for g in range(draft + 1):
        rs = pl.ds(g * batch, batch)
        m = m_ref[rs, :]
        top = jnp.max(m, axis=1, keepdims=True)
        tot = jnp.sum(l_ref[rs, :] * jnp.exp2(m - top), axis=1, keepdims=True)
        msg1[pl.ds(g, 1), pl.ds(0, batch)] = _col_to_row(top + jnp.log2(tot))

    def token_rows(src, dst):
        @pl.loop(0, batch, unroll=4)
        def _(b):
            for j in range(draft):
                idx = tok_smem[j, b] - me * vocab
                idx = jnp.minimum(jnp.maximum(idx, 0), vocab - 1)
                c = lax.shift_right_logical(idx, 7)
                dst[pl.ds(j * batch + b, 1), :] = src[c, pl.ds(b * draft + j, 1), :]

    token_rows(q_ref, gq_buf)
    pl.semaphore_wait(barrier, ntp - 1)
    for d in range(1, ntp):
        remote(msg1, got1, send1, recv1, d).start()
    got1[me] = msg1[...]

    token_rows(s_ref, gs_buf)
    msg2[...] = jnp.zeros_like(msg2)
    lane = lax.broadcasted_iota(jnp.int32, (batch, LANES), 1)
    for j in range(draft):
        idx = _row_to_col(tok_ref[pl.ds(j, 1), :].astype(jnp.float32)).astype(jnp.int32) - me * vocab
        owned = jnp.logical_and(idx >= 0, idx < vocab)
        hit = jnp.logical_and(owned, lane == jnp.bitwise_and(idx, LANES - 1))
        rs = pl.ds(j * batch, batch)
        tok_s = jnp.sum(jnp.where(hit, gs_buf[rs, :], 0.0), axis=1, keepdims=True)
        tok_q = jnp.sum(jnp.where(hit, gq_buf[rs, :], 0.0), axis=1, keepdims=True)
        msg2[pl.ds(draft + j, 1), pl.ds(0, batch)] = _col_to_row(tok_s)
        msg2[pl.ds(2 * draft + j, 1), pl.ds(0, batch)] = _col_to_row(tok_q)

    for d in range(1, ntp):
        arrived(msg1, got1, send1, recv1, d).wait_recv()
    top = got1[0]
    for i in range(1, ntp):
        top = jnp.maximum(top, got1[i])
    tot = jnp.exp2(got1[0] - top)
    for i in range(1, ntp):
        tot = tot + jnp.exp2(got1[i] - top)
    lse2 = top + jnp.log2(tot)
    bonus_ref[...] = lse2[draft:draft + 1, 0:batch] * LN2
    for j in range(draft):
        col_buf[pl.ds(j, batch, stride=draft), :] = jnp.broadcast_to(
            _row_to_col(lse2[j:j + 1, 0:batch]), (batch, LANES))

    nv = batch * draft // 8
    last_mask = lax.broadcasted_iota(jnp.int32, (8, LANES), 1) < last

    @pl.loop(0, nv // 2)
    def _(v):
        rss = [pl.ds(pl.multiple_of((2 * v + i) * 8, 8), 8) for i in range(2)]
        ls = [col_buf[rs, :] for rs in rss]

        def ex(c, i):
            return jnp.maximum(jnp.exp2(s_ref[c, rss[i], :] - ls[i]) - q_ref[c, rss[i], :], 0.0)

        sums = [[jnp.zeros((8, LANES), jnp.float32) for _ in range(4)] for _ in range(2)]
        for c in range(nc - 1):
            for i in range(2):
                sums[i][c % 4] = sums[i][c % 4] + ex(c, i)
        sums = [(a + b) + (c + d) for a, b, c, d in sums]
        for i in range(2):
            e = jnp.where(last_mask, ex(nc - 1, i), 0.0)
            part_buf[rss[i], :] = sums[i] + e

    for j in range(draft):
        part = jnp.sum(part_buf[pl.ds(j, batch, stride=draft), :], axis=1, keepdims=True)
        msg2[pl.ds(j, 1), pl.ds(0, batch)] = _col_to_row(part)

    for d in range(1, ntp):
        remote(msg2, got2, send2, recv2, d).start()
    got2[me] = msg2[...]
    for d in range(1, ntp):
        arrived(msg2, got2, send2, recv2, d).wait_recv()
    tot = got2[0]
    for i in range(1, ntp):
        tot = tot + got2[i]
    norm = tot[0:draft, 0:batch]
    norm_ref[...] = norm
    target = jnp.exp2(tot[draft:2 * draft, 0:batch] - lse2[0:draft, 0:batch])
    accept_ref[...] = jnp.minimum(1.0, target / tot[2 * draft:3 * draft, 0:batch])
    for j in range(draft):
        inv_ref[pl.ds(j, batch, stride=draft), :] = jnp.broadcast_to(
            1.0 / _row_to_col(norm[j:j + 1, :]), (batch, LANES))
    for d in range(1, ntp):
        remote(msg1, got1, send1, recv1, d).wait_send()
        remote(msg2, got2, send2, recv2, d).wait_send()


OUT_GROUP = 5


def _write_kernel(
    dims, s_ref, q_ref, lse_ref, inv_ref, accept_in, norm_in, bonus_in,
    out_hbm, accept_ref, norm_ref, bonus_ref, stage, stage_last, sem,
):
    batch, draft, vocab = dims
    nc = -(-vocab // LANES)
    last = vocab - (nc - 1) * LANES
    view = stage.reshape(nc, batch, draft, LANES)
    ngroups = (nc - 1) // OUT_GROUP
    assert ngroups * OUT_GROUP == nc - 1

    def copy(c):
        return pltpu.make_async_copy(
            view.at[c], out_hbm.at[:, :, pl.ds(pl.multiple_of(c * LANES, LANES), LANES)], sem.at[0])

    def fill(c):
        stage[c] = jnp.maximum(jnp.exp2(s_ref[c] - lse_ref[...]) - q_ref[c], 0.0) * inv_ref[...]

    fill(nc - 1)
    for b in range(batch):
        stage_last[b] = stage[nc - 1, pl.ds(b * draft, draft), pl.ds(0, last)]
    last_copy = pltpu.make_async_copy(stage_last, out_hbm.at[:, :, pl.ds((nc - 1) * LANES, last)], sem.at[1])
    last_copy.start()

    @pl.loop(0, ngroups)
    def _(t):
        for i in range(OUT_GROUP):
            fill(t * OUT_GROUP + i)
            copy(t * OUT_GROUP + i).start()

    accept_ref[...] = accept_in[...]
    norm_ref[...] = norm_in[...]
    bonus_ref[...] = bonus_in[...]
    last_copy.wait()
    bulk = stage.at[pl.ds(0, nc - 1)]
    pltpu.make_async_copy(bulk, bulk, sem.at[0]).wait()


def solution(mesh):
    ntp = mesh.shape["tp"]

    def local_step(hidden, norm_gain, w_head, draft_probs, draft_tokens, temperature):
        batch, draft, vocab = draft_probs.shape
        depth = hidden.shape[2]
        rows = batch * (draft + 1)
        nc = -(-vocab // LANES)
        vmem = pl.BlockSpec(memory_space=pltpu.VMEM)
        hbm = pl.BlockSpec(memory_space=pl.ANY)
        smem = pl.BlockSpec(memory_space=pltpu.SMEM)
        keep = functools.partial(pltpu.with_memory_space_constraint, memory_space=pltpu.VMEM)
        f32, bf16, dma = jnp.float32, jnp.bfloat16, pltpu.SemaphoreType.DMA
        vec = pltpu.VMEM((batch * draft, LANES), f32)
        big = pltpu.VMEM((nc, batch * draft, LANES), f32)
        stat = pltpu.VMEM((rows, LANES), f32)
        x = hidden.transpose(1, 0, 2).reshape(rows, depth)
        tok = draft_tokens.T
        s, q, m, l = pl.pallas_call(
            functools.partial(_logits_kernel, (batch, draft, depth, vocab)),
            out_shape=(big, big, stat, stat),
            in_specs=[hbm, vmem, hbm, hbm, vmem],
            out_specs=(vmem,) * 4,
            scratch_shapes=[
                pltpu.VMEM((rows, depth), bf16),
                pltpu.VMEM((rows, depth), bf16),
                pltpu.VMEM((RING, STEP, depth), bf16),
                pltpu.VMEM((batch, draft, vocab - (nc - 1) * LANES), f32),
                pltpu.VMEM((batch, LANES), f32),
                dma,
                dma((RING, W_PARTS)),
                dma((2,)),
                pltpu.SemaphoreType.REGULAR,
            ],
            compiler_params=pltpu.CompilerParams(vmem_limit_bytes=GRANT),
            name="logits",
        )(x, norm_gain.reshape(1, depth), w_head.T, draft_probs, temperature.reshape(1, batch))
        lse, inv, accept, norm, bonus = pl.pallas_call(
            functools.partial(_verify_kernel, (batch, draft, vocab, ntp)),
            out_shape=(
                vec,
                vec,
                pltpu.VMEM((draft, batch), f32),
                pltpu.VMEM((draft, batch), f32),
                pltpu.VMEM((1, batch), f32),
            ),
            in_specs=[vmem, vmem, vmem, vmem, smem, vmem],
            out_specs=(vmem,) * 5,
            scratch_shapes=[
                vec, vec, vec,
                pltpu.VMEM((8, LANES), f32),
                pltpu.VMEM((16, LANES), f32),
                pltpu.VMEM((ntp, 8, LANES), f32),
                pltpu.VMEM((ntp, 16, LANES), f32),
                dma((ntp,)), dma((ntp,)), dma((ntp,)), dma((ntp,)),
            ],
            compiler_params=pltpu.CompilerParams(
                collective_id=0, has_side_effects=True, vmem_limit_bytes=GRANT),
            name="verify",
        )(keep(s), keep(q), keep(m), keep(l), tok, tok)
        residual, accept, norm, bonus = pl.pallas_call(
            functools.partial(_write_kernel, (batch, draft, vocab)),
            out_shape=(
                jax.ShapeDtypeStruct(draft_probs.shape, f32),
                jax.ShapeDtypeStruct((draft, batch), f32),
                jax.ShapeDtypeStruct((draft, batch), f32),
                jax.ShapeDtypeStruct((1, batch), f32),
            ),
            in_specs=[vmem] * 7,
            out_specs=(hbm, vmem, vmem, vmem),
            scratch_shapes=[
                big,
                pltpu.VMEM((batch, draft, vocab - (nc - 1) * LANES), f32),
                dma((2,)),
            ],
            compiler_params=pltpu.CompilerParams(vmem_limit_bytes=GRANT),
            name="write",
        )(*map(keep, (s, q, lse, inv, accept, norm, bonus)))
        return accept.T, norm.T, residual, bonus.reshape(batch)

    return jax.shard_map(
        local_step,
        mesh=mesh,
        in_specs=(P('dp', None, None), P(), P(None, 'tp'), P('dp', None, 'tp'), P('dp', None), P('dp')),
        out_specs=(P('dp', None), P('dp', None), P('dp', None, 'tp'), P('dp')),
        check_vma=False,
    )
```

```python
import functools

import jax
import jax.numpy as jnp
from jax import lax
from jax.experimental import pallas as pl
from jax.experimental.pallas import tpu as pltpu
from jax.sharding import PartitionSpec as P

LANES = 128
TILE = 256
STEP = 2 * TILE
RING = 8
SLAB = 64
CHUNK = 25
W_PARTS = 4
FENCES = 6
Q_LATE = 5
TOK_STEP = 8
SIG = (1, 3, 5, 7)
GRP = {1: (0,), 3: (1, 2), 5: (3, 4)}
GRANT = 24 * 1024 * 1024
LOG2E = 1.4426950408889634
LN2 = 0.6931471805599453
LOWEST = -3.4028234e38
MESH = pl.DeviceIdType.MESH


def _row_to_col(row):
    n = row.shape[1]
    r = lax.broadcasted_iota(jnp.int32, (n, n), 0)
    c = lax.broadcasted_iota(jnp.int32, (n, n), 1)
    return jnp.sum(jnp.where(r == c, row, 0.0), axis=1, keepdims=True)


def _col_to_row(col):
    n = col.shape[0]
    r = lax.broadcasted_iota(jnp.int32, (n, n), 0)
    c = lax.broadcasted_iota(jnp.int32, (n, n), 1)
    return jnp.sum(jnp.where(r == c, col, 0.0), axis=0, keepdims=True)


def _q_first(vocab):
    return (vocab // LANES) * Q_LATE // 8


def _logits_kernel(
    dims,
    x_hbm, gain_ref, w_hbm, q_hbm, temp_ref, tok_smem,
    s_ref, q_buf, m_buf, l_buf, tile_ref,
    h_buf, x_buf, w_buf, q_last, scale_buf,
    h_sem, w_sem, q_sem, fence,
):
    batch, draft, depth, vocab = dims
    tokens = batch * draft
    me = lax.axis_index("tp")
    q_first = _q_first(vocab)
    rows = batch * (draft + 1)
    nk = depth // TILE
    full = vocab // STEP
    rest = vocab - full * STEP
    nc = -(-vocab // LANES)
    last = vocab - (nc - 1) * LANES
    part = STEP // W_PARTS

    def w_copy(n, i, size=part):
        slot = lax.rem(n, RING)
        return pltpu.make_async_copy(
            w_hbm.at[pl.ds(n * STEP + i * part, size), :], w_buf.at[slot, pl.ds(i * part, size), :], w_sem.at[slot, i])

    def w_wait(n):
        for i in range(W_PARTS):
            w_copy(n, i).wait()

    def w_rest():
        return [w_copy(full, i, min(part, rest - i * part)) for i in range(-(-rest // part))]

    tiles = tile_ref.reshape(tokens, draft, LANES)
    qv = q_buf.reshape(nc, batch, draft, LANES)

    def q_copy(c):
        return pltpu.make_async_copy(
            q_hbm.at[:, :, pl.ds(pl.multiple_of(c * LANES, LANES), LANES)], qv.at[c], q_sem.at[0])

    def token_copy(b, j):
        idx = tok_smem[j, b] - me * vocab
        c = lax.shift_right_logical(jnp.minimum(jnp.maximum(idx, 0), vocab - 1), 7)
        c = jnp.minimum(c, nc - 2)
        return pltpu.make_async_copy(
            q_hbm.at[b, :, pl.ds(pl.multiple_of(c * LANES, LANES), LANES)], tiles.at[b * draft + j], q_sem.at[2])

    def last_q():
        return pltpu.make_async_copy(
            q_hbm.at[:, :, pl.ds((nc - 1) * LANES, last)], q_last, q_sem.at[1])

    h_copy = pltpu.make_async_copy(x_hbm, h_buf, h_sem)
    h_copy.start()
    for n in range(RING - 1):
        for i in range(W_PARTS):
            w_copy(n, i).start()
    last_q().start(priority=1)

    temp_col = _row_to_col(temp_ref[...])
    scale_buf[...] = jnp.broadcast_to(LOG2E / temp_col, (batch, LANES))
    m_buf[...] = jnp.full_like(m_buf, LOWEST)
    l_buf[...] = jnp.zeros_like(l_buf)

    groups = draft + 1

    def online(g, q, c0, z, ncol, penalty=None):
        rs = pl.ds(g * batch, batch)
        scale = scale_buf[...]
        ss = [z[:, i * LANES:(i + 1) * LANES] * scale for i in range(ncol)]
        if penalty is not None:
            ss = [s + p for s, p in zip(ss, penalty)]
        m_old = m_buf[rs, :]
        m_new = m_old
        for s in ss:
            m_new = jnp.maximum(m_new, s)
        l = l_buf[rs, :] * jnp.exp2(m_old - m_new)
        for s in ss:
            l = l + jnp.exp2(s - m_new)
        m_buf[rs, :] = m_new
        l_buf[rs, :] = l
        if g < draft:
            for i in range(ncol):
                s_ref[c0 + i, pl.ds(g, batch, stride=draft), :] = ss[i]

    def lhs(g, k):
        return x_buf[pl.ds(g * batch, batch), pl.ds(k * TILE, TILE)]

    def push(n, q, k):
        slot = lax.rem(n, RING)
        w = w_buf[slot, pl.ds(q * TILE, TILE), pl.ds(k * TILE, TILE)]
        pltpu.matmul_push_rhs(w, staging_register=k % 2, mxu_index=q, transpose=True)

    def mxu_body(*accs):
        acc = [[[accs[(a * 2 + q) * groups + g] for g in range(groups)] for q in range(2)] for a in range(2)]
        for a in range(2):
            for q in range(2):
                for g in range(groups):
                    pltpu.matmul_pop(acc[a][q][g])

        h_copy.wait()
        for i in range(rows // 32):
            sl = pl.ds(i * 32, 32)
            h = h_buf[sl, :].astype(jnp.float32)
            r = lax.rsqrt(jnp.mean(h * h, axis=-1, keepdims=True) + 1e-5)
            x_buf[sl, :] = (h_buf[sl, :].astype(jnp.float32) * r * gain_ref[...]).astype(jnp.bfloat16)

        half = nk // 2

        def push_rest(q, kk):
            w = w_buf[full % RING, pl.ds(0, TILE), pl.ds((q * half + kk) * TILE, TILE)]
            pltpu.matmul_push_rhs(w, staging_register=kk % 2, mxu_index=q, transpose=True)

        def fullstep(n, a, issue, penalty=None, next_full=True):
            old = acc[1 - a]
            c_old = jnp.maximum(n - 1, 0) * (STEP // LANES)
            for k in range(nk):
                for q in range(2):
                    for g in range(groups):
                        pltpu.matmul_acc_lhs(acc[a][q][g], lhs(g, k), load_staged_rhs=k % 2 if g == 0 else None)
                for q in range(2):
                    if k + 1 < nk:
                        push(n, q, k + 1)
                    elif next_full:
                        push(n + 1, q, 0)
                    else:
                        push_rest(q, 0)
                if 1 <= k <= FENCES:
                    issue(k - 1)
                if k in SIG:
                    pl.semaphore_signal(fence, 1)
                for g in GRP.get(k, ()):
                    for q in range(2):
                        z = pltpu.matmul_pop(old[q][g])
                        online(g, q, c_old + q * (TILE // LANES), z, TILE // LANES,
                               None if penalty is None else [penalty] * (TILE // LANES))

            pl.semaphore_wait(fence, len(SIG))

        w_wait(0)
        for q in range(2):
            push(0, q, 0)

        split = (full - (RING - 1)) // 2 * 2
        tail = full // 2 * 2
        early = 1
        mid = nc - 1 - q_first - early * split
        assert mid >= 0 and tail == full - 1 and tokens >= TOK_STEP * full

        def issue_tokens(n):
            for i in range(TOK_STEP):
                token_copy(n * (TOK_STEP // draft) + i // draft, i % draft).start(priority=1)

        def issue_early(n, i):
            if i < W_PARTS:
                w_copy(n + RING - 1, i).start()
            elif i == W_PARTS:
                q_copy(q_first + n).start(priority=1)
            else:
                issue_tokens(n)

        def issue_late(n, i):
            if i == W_PARTS + 1:
                issue_tokens(n)

        @pl.loop(0, split // 2)
        def _(t):
            n = 2 * t
            w_wait(n + 1)
            fullstep(n, 0, lambda i: issue_early(n, i), penalty=jnp.where(t == 0, LOWEST, 0.0).astype(jnp.float32))
            w_wait(n + 2)
            fullstep(n + 1, 1, lambda i: issue_early(n + 1, i))

        for copy in w_rest():
            copy.start()

        @pl.loop(0, mid)
        def _(i):
            q_copy(q_first + early * split + i).start(priority=1)

        for i in range(TOK_STEP * full, tokens):
            token_copy(i // draft, i % draft).start(priority=1)

        @pl.loop(split // 2, tail // 2)
        def _(t):
            n = 2 * t
            w_wait(n + 1)
            fullstep(n, 0, lambda i: issue_late(n, i))
            w_wait(n + 2)
            fullstep(n + 1, 1, lambda i: issue_late(n + 1, i))

        n = full - 1
        for copy in w_rest():
            copy.wait()
        last_q().wait()
        for b in range(0, batch, 2):
            q_buf[nc - 1, pl.ds(b * draft, 2 * draft), pl.ds(0, last)] = jnp.concatenate([q_last[b], q_last[b + 1]], axis=0)
        fullstep(n, 0, lambda i: issue_late(n, i), next_full=False)
        for kk in range(half):
            for q in range(2):
                for g in range(groups):
                    pltpu.matmul_acc_lhs(acc[1][q][g], lhs(g, q * half + kk), load_staged_rhs=kk % 2 if g == 0 else None)
                if kk + 1 < half:
                    push_rest(q, kk + 1)
        for g in range(groups):
            for q in range(2):
                z = pltpu.matmul_pop(acc[0][q][g])
                online(g, q, n * (STEP // LANES) + q * (TILE // LANES), z, TILE // LANES)
        ncol = -(-rest // LANES)
        lane = lax.broadcasted_iota(jnp.int32, (batch, LANES), 1)
        pens = [None] * ncol
        for i in range(ncol):
            pens[i] = jnp.where(lane + i * LANES < rest, 0.0, LOWEST)
        for g in range(groups):
            z = pltpu.matmul_pop(acc[1][0][g]) + pltpu.matmul_pop(acc[1][1][g])
            online(g, 0, full * (STEP // LANES), z, ncol, pens)

    specs = [pltpu.ACC(q)((batch, TILE), jnp.float32) for a in range(2) for q in range(2) for g in range(groups)]
    pl.run_scoped(mxu_body, *specs)

    bulk = q_buf.at[pl.ds(q_first, nc - 1 - q_first)]
    pltpu.make_async_copy(bulk, bulk, q_sem.at[0]).wait()
    pltpu.make_async_copy(tile_ref, tile_ref, q_sem.at[2]).wait()


def _verify_kernel(
    dims,
    s_ref, q_in, m_ref, l_ref, tile_ref, tok_smem, tok_ref, q_hbm,
    q_ref, col_buf, inv_ref, accept_ref, norm_ref, bonus_ref,
    gs_buf, part_buf,
    msg1, msg2, got1, got2,
    send1, recv1, send2, recv2, q_sem,
):
    del q_in
    batch, draft, vocab, ntp = dims
    nc = -(-vocab // LANES)
    last = vocab - (nc - 1) * LANES
    me = lax.axis_index("tp")
    barrier = pltpu.get_barrier_semaphore()
    for d in range(1, ntp):
        pl.semaphore_signal(barrier, inc=1, device_id={"tp": lax.rem(me + d, ntp)}, device_id_type=MESH)
    q_first = _q_first(vocab)
    qv = q_ref.reshape(nc, batch, draft, LANES)

    def q_copy(c):
        return pltpu.make_async_copy(
            q_hbm.at[:, :, pl.ds(pl.multiple_of(c * LANES, LANES), LANES)], qv.at[c], q_sem.at[c])

    @pl.loop(0, q_first)
    def _(c):
        q_copy(c).start()

    def remote(msg, got, send, recv, d):
        return pltpu.make_async_remote_copy(
            src_ref=msg, dst_ref=got.at[me], send_sem=send.at[d], recv_sem=recv.at[me],
            device_id={"tp": lax.rem(me + d, ntp)}, device_id_type=MESH)

    def arrived(msg, got, send, recv, d):
        src = lax.rem(me + d, ntp)
        return pltpu.make_async_remote_copy(
            src_ref=msg, dst_ref=got.at[src], send_sem=send.at[d], recv_sem=recv.at[src],
            device_id={"tp": src}, device_id_type=MESH)

    msg1[...] = jnp.zeros_like(msg1)
    for g in range(draft + 1):
        rs = pl.ds(g * batch, batch)
        m = m_ref[rs, :]
        top = jnp.max(m, axis=1, keepdims=True)
        tot = jnp.sum(l_ref[rs, :] * jnp.exp2(m - top), axis=1, keepdims=True)
        msg1[pl.ds(g, 1), pl.ds(0, batch)] = _col_to_row(top + jnp.log2(tot))

    def token_rows(src, dst):
        @pl.loop(0, batch, unroll=4)
        def _(b):
            for j in range(draft):
                idx = tok_smem[j, b] - me * vocab
                idx = jnp.minimum(jnp.maximum(idx, 0), vocab - 1)
                c = lax.shift_right_logical(idx, 7)
                dst[pl.ds(j * batch + b, 1), :] = src[c, pl.ds(b * draft + j, 1), :]

    pl.semaphore_wait(barrier, ntp - 1)
    for d in range(1, ntp):
        remote(msg1, got1, send1, recv1, d).start()
    got1[me] = msg1[...]

    token_rows(s_ref, gs_buf)
    msg2[...] = jnp.zeros_like(msg2)
    lane = lax.broadcasted_iota(jnp.int32, (batch, LANES), 1)
    for j in range(draft):
        idx = _row_to_col(tok_ref[pl.ds(j, 1), :].astype(jnp.float32)).astype(jnp.int32) - me * vocab
        owned = jnp.logical_and(idx >= 0, idx < vocab)
        hit = jnp.logical_and(owned, lane == jnp.bitwise_and(idx, LANES - 1))
        rs = pl.ds(j * batch, batch)
        tok_s = jnp.sum(jnp.where(hit, gs_buf[rs, :], 0.0), axis=1, keepdims=True)
        q_row = jnp.where(
            lax.shift_right_logical(idx, 7) == nc - 1,
            q_ref[nc - 1, pl.ds(j, batch, stride=draft), :],
            tile_ref[pl.ds((draft + 1) * j, batch, stride=draft * draft), :])
        tok_q = jnp.sum(jnp.where(hit, q_row, 0.0), axis=1, keepdims=True)
        msg2[pl.ds(draft + j, 1), pl.ds(0, batch)] = _col_to_row(tok_s)
        msg2[pl.ds(2 * draft + j, 1), pl.ds(0, batch)] = _col_to_row(tok_q)

    for d in range(1, ntp):
        arrived(msg1, got1, send1, recv1, d).wait_recv()
    top = got1[0]
    for i in range(1, ntp):
        top = jnp.maximum(top, got1[i])
    tot = jnp.exp2(got1[0] - top)
    for i in range(1, ntp):
        tot = tot + jnp.exp2(got1[i] - top)
    lse2 = top + jnp.log2(tot)
    bonus_ref[...] = lse2[draft:draft + 1, 0:batch] * LN2
    for j in range(draft):
        col_buf[pl.ds(j, batch, stride=draft), :] = jnp.broadcast_to(
            _row_to_col(lse2[j:j + 1, 0:batch]), (batch, LANES))

    @pl.loop(0, q_first)
    def _(c):
        q_copy(c).wait()

    last_mask = lax.broadcasted_iota(jnp.int32, (SLAB, LANES), 1) < last

    @pl.loop(0, batch * draft // SLAB)
    def _(v):
        rs = pl.ds(pl.multiple_of(v * SLAB, SLAB), SLAB)
        lse = col_buf[rs, :]

        def ex(c):
            return jnp.maximum(jnp.exp2(s_ref[c, rs, :] - lse) - q_ref[c, rs, :], 0.0)

        def chunk(t, total):
            for i in range(CHUNK):
                total = total + ex(t * CHUNK + i)
            return total

        part_buf[rs, :] = lax.fori_loop(
            0, (nc - 1) // CHUNK, chunk, jnp.where(last_mask, ex(nc - 1), 0.0))

    for j in range(draft):
        part = jnp.sum(part_buf[pl.ds(j, batch, stride=draft), :], axis=1, keepdims=True)
        msg2[pl.ds(j, 1), pl.ds(0, batch)] = _col_to_row(part)

    for d in range(1, ntp):
        remote(msg2, got2, send2, recv2, d).start()
    got2[me] = msg2[...]
    for d in range(1, ntp):
        arrived(msg2, got2, send2, recv2, d).wait_recv()
    tot = got2[0]
    for i in range(1, ntp):
        tot = tot + got2[i]
    norm = tot[0:draft, 0:batch]
    norm_ref[...] = norm
    target = jnp.exp2(tot[draft:2 * draft, 0:batch] - lse2[0:draft, 0:batch])
    accept_ref[...] = jnp.minimum(1.0, target / tot[2 * draft:3 * draft, 0:batch])
    for j in range(draft):
        inv_ref[pl.ds(j, batch, stride=draft), :] = jnp.broadcast_to(
            1.0 / _row_to_col(norm[j:j + 1, :]), (batch, LANES))
    for d in range(1, ntp):
        remote(msg1, got1, send1, recv1, d).wait_send()
        remote(msg2, got2, send2, recv2, d).wait_send()


OUT_GROUP = 5


def _write_kernel(
    dims, s_ref, q_ref, lse_ref, inv_ref, accept_in, norm_in, bonus_in,
    out_hbm, accept_ref, norm_ref, bonus_ref, stage, stage_last, sem,
):
    batch, draft, vocab = dims
    nc = -(-vocab // LANES)
    last = vocab - (nc - 1) * LANES
    view = stage.reshape(nc, batch, draft, LANES)
    ngroups = (nc - 1) // OUT_GROUP
    assert ngroups * OUT_GROUP == nc - 1

    def copy(c):
        return pltpu.make_async_copy(
            view.at[c], out_hbm.at[:, :, pl.ds(pl.multiple_of(c * LANES, LANES), LANES)], sem.at[0])

    def fill(c):
        stage[c] = jnp.maximum(jnp.exp2(s_ref[c] - lse_ref[...]) - q_ref[c], 0.0) * inv_ref[...]

    fill(nc - 1)
    for b in range(batch):
        stage_last[b] = stage[nc - 1, pl.ds(b * draft, draft), pl.ds(0, last)]
    last_copy = pltpu.make_async_copy(stage_last, out_hbm.at[:, :, pl.ds((nc - 1) * LANES, last)], sem.at[1])
    last_copy.start()

    @pl.loop(0, ngroups)
    def _(t):
        for i in range(OUT_GROUP):
            fill(t * OUT_GROUP + i)
            copy(t * OUT_GROUP + i).start()

    accept_ref[...] = accept_in[...]
    norm_ref[...] = norm_in[...]
    bonus_ref[...] = bonus_in[...]
    last_copy.wait()
    bulk = stage.at[pl.ds(0, nc - 1)]
    pltpu.make_async_copy(bulk, bulk, sem.at[0]).wait()


def solution(mesh):
    ntp = mesh.shape["tp"]

    def local_step(hidden, norm_gain, w_head, draft_probs, draft_tokens, temperature):
        batch, draft, vocab = draft_probs.shape
        depth = hidden.shape[2]
        rows = batch * (draft + 1)
        nc = -(-vocab // LANES)
        vmem = pl.BlockSpec(memory_space=pltpu.VMEM)
        hbm = pl.BlockSpec(memory_space=pl.ANY)
        smem = pl.BlockSpec(memory_space=pltpu.SMEM)
        keep = functools.partial(pltpu.with_memory_space_constraint, memory_space=pltpu.VMEM)
        f32, bf16, dma = jnp.float32, jnp.bfloat16, pltpu.SemaphoreType.DMA
        vec = pltpu.VMEM((batch * draft, LANES), f32)
        big = pltpu.VMEM((nc, batch * draft, LANES), f32)
        stat = pltpu.VMEM((rows, LANES), f32)
        x = hidden.transpose(1, 0, 2).reshape(rows, depth)
        tok = draft_tokens.T
        s, q, m, l, tiles = pl.pallas_call(
            functools.partial(_logits_kernel, (batch, draft, depth, vocab)),
            out_shape=(big, big, stat, stat, pltpu.VMEM((batch * draft * draft, LANES), f32)),
            in_specs=[hbm, vmem, hbm, hbm, vmem, smem],
            out_specs=(vmem,) * 5,
            scratch_shapes=[
                pltpu.VMEM((rows, depth), bf16),
                pltpu.VMEM((rows, depth), bf16),
                pltpu.VMEM((RING, STEP, depth), bf16),
                pltpu.VMEM((batch, draft, vocab - (nc - 1) * LANES), f32),
                pltpu.VMEM((batch, LANES), f32),
                dma,
                dma((RING, W_PARTS)),
                dma((3,)),
                pltpu.SemaphoreType.REGULAR,
            ],
            compiler_params=pltpu.CompilerParams(vmem_limit_bytes=GRANT),
            name="logits",
        )(x, norm_gain.reshape(1, depth), w_head.T, draft_probs, temperature.reshape(1, batch), tok)
        q, lse, inv, accept, norm, bonus = pl.pallas_call(
            functools.partial(_verify_kernel, (batch, draft, vocab, ntp)),
            out_shape=(
                big,
                vec,
                vec,
                pltpu.VMEM((draft, batch), f32),
                pltpu.VMEM((draft, batch), f32),
                pltpu.VMEM((1, batch), f32),
            ),
            in_specs=[vmem, vmem, vmem, vmem, vmem, smem, vmem, hbm],
            out_specs=(vmem,) * 6,
            input_output_aliases={1: 0},
            scratch_shapes=[
                vec, vec,
                pltpu.VMEM((8, LANES), f32),
                pltpu.VMEM((16, LANES), f32),
                pltpu.VMEM((ntp, 8, LANES), f32),
                pltpu.VMEM((ntp, 16, LANES), f32),
                dma((ntp,)), dma((ntp,)), dma((ntp,)), dma((ntp,)), dma((nc,)),
            ],
            compiler_params=pltpu.CompilerParams(
                collective_id=0, has_side_effects=True, vmem_limit_bytes=GRANT),
            name="verify",
        )(keep(s), keep(q), keep(m), keep(l), keep(tiles), tok, tok, draft_probs)
        residual, accept, norm, bonus = pl.pallas_call(
            functools.partial(_write_kernel, (batch, draft, vocab)),
            out_shape=(
                jax.ShapeDtypeStruct(draft_probs.shape, f32),
                jax.ShapeDtypeStruct((draft, batch), f32),
                jax.ShapeDtypeStruct((draft, batch), f32),
                jax.ShapeDtypeStruct((1, batch), f32),
            ),
            in_specs=[vmem] * 7,
            out_specs=(hbm, vmem, vmem, vmem),
            scratch_shapes=[
                big,
                pltpu.VMEM((batch, draft, vocab - (nc - 1) * LANES), f32),
                dma((2,)),
            ],
            compiler_params=pltpu.CompilerParams(vmem_limit_bytes=GRANT),
            name="write",
        )(*map(keep, (s, q, lse, inv, accept, norm, bonus)))
        return accept.T, norm.T, residual, bonus.reshape(batch)

    return jax.shard_map(
        local_step,
        mesh=mesh,
        in_specs=(P('dp', None, None), P(), P(None, 'tp'), P('dp', None, 'tp'), P('dp', None), P('dp')),
        out_specs=(P('dp', None), P('dp', None), P('dp', None, 'tp'), P('dp')),
        check_vma=False,
    )
```

```python
import functools

import jax
import jax.numpy as jnp
from jax import lax
from jax.experimental import pallas as pl
from jax.experimental.pallas import tpu as pltpu
from jax.sharding import PartitionSpec as P

LANES = 128
TILE = 256
STEP = 2 * TILE
RING = 8
SLAB = 64
CHUNK = 25
W_PARTS = 4
FENCES = 6
Q_LATE = 5
TOK_STEP = 8
SIG = (1, 3, 5, 7)
GRP = {1: (0,), 3: (1, 2), 5: (3, 4)}
GRANT = 24 * 1024 * 1024
LOG2E = 1.4426950408889634
LN2 = 0.6931471805599453
LOWEST = -3.4028234e38
MESH = pl.DeviceIdType.MESH


def _row_to_col(row):
    n = row.shape[1]
    r = lax.broadcasted_iota(jnp.int32, (n, n), 0)
    c = lax.broadcasted_iota(jnp.int32, (n, n), 1)
    return jnp.sum(jnp.where(r == c, row, 0.0), axis=1, keepdims=True)


def _col_to_row(col):
    n = col.shape[0]
    r = lax.broadcasted_iota(jnp.int32, (n, n), 0)
    c = lax.broadcasted_iota(jnp.int32, (n, n), 1)
    return jnp.sum(jnp.where(r == c, col, 0.0), axis=0, keepdims=True)


def _q_first(vocab):
    return (vocab // LANES) * Q_LATE // 8


def _logits_kernel(
    dims,
    x_hbm, gain_hbm, w_hbm, q_hbm, temp_hbm, tok_hbm,
    s_ref, q_buf, m_buf, l_buf, tile_ref,
    h_buf, x_buf, w_buf, q_last, scale_buf, gain_ref, temp_ref, tok_smem,
    h_sem, w_sem, q_sem, small_sem, fence,
):
    batch, draft, depth, vocab = dims
    tokens = batch * draft
    me = lax.axis_index("tp")
    q_first = _q_first(vocab)
    rows = batch * (draft + 1)
    nk = depth // TILE
    full = vocab // STEP
    rest = vocab - full * STEP
    nc = -(-vocab // LANES)
    last = vocab - (nc - 1) * LANES
    part = STEP // W_PARTS

    def w_copy(n, i, size=part):
        slot = lax.rem(n, RING)
        return pltpu.make_async_copy(
            w_hbm.at[pl.ds(n * STEP + i * part, size), :], w_buf.at[slot, pl.ds(i * part, size), :], w_sem.at[slot, i])

    def w_wait(n):
        for i in range(W_PARTS):
            w_copy(n, i).wait()

    def w_rest():
        return [w_copy(full, i, min(part, rest - i * part)) for i in range(-(-rest // part))]

    tiles = tile_ref.reshape(tokens, draft, LANES)
    qv = q_buf.reshape(nc, batch, draft, LANES)

    def q_copy(c):
        return pltpu.make_async_copy(
            q_hbm.at[:, :, pl.ds(pl.multiple_of(c * LANES, LANES), LANES)], qv.at[c], q_sem.at[0])

    def token_copy(b, j):
        idx = tok_smem[j, b] - me * vocab
        c = lax.shift_right_logical(jnp.minimum(jnp.maximum(idx, 0), vocab - 1), 7)
        c = jnp.minimum(c, nc - 2)
        return pltpu.make_async_copy(
            q_hbm.at[b, :, pl.ds(pl.multiple_of(c * LANES, LANES), LANES)], tiles.at[b * draft + j], q_sem.at[2])

    def last_q():
        return pltpu.make_async_copy(
            q_hbm.at[:, :, pl.ds((nc - 1) * LANES, last)], q_last, q_sem.at[1])

    def h_copy(g):
        rs = pl.ds(g * batch, batch)
        return pltpu.make_async_copy(x_hbm.at[rs, :], h_buf.at[rs, :], h_sem.at[g])

    small = [
        pltpu.make_async_copy(src, dst, small_sem.at[i])
        for i, (src, dst) in enumerate([(gain_hbm, gain_ref), (temp_hbm, temp_ref), (tok_hbm, tok_smem)])
    ]
    for g in range(draft + 1):
        h_copy(g).start()
    for copy in small:
        copy.start()
    for n in range(RING - 1):
        for i in range(W_PARTS):
            w_copy(n, i).start(priority=i % 2)
    last_q().start(priority=1)

    m_buf[...] = jnp.full_like(m_buf, LOWEST)
    l_buf[...] = jnp.zeros_like(l_buf)

    groups = draft + 1

    def online(g, q, c0, z, ncol, penalty=None):
        rs = pl.ds(g * batch, batch)
        scale = scale_buf[...]
        ss = [z[:, i * LANES:(i + 1) * LANES] * scale for i in range(ncol)]
        if penalty is not None:
            ss = [s + p for s, p in zip(ss, penalty)]
        m_old = m_buf[rs, :]
        m_new = m_old
        for s in ss:
            m_new = jnp.maximum(m_new, s)
        l = l_buf[rs, :] * jnp.exp2(m_old - m_new)
        for s in ss:
            l = l + jnp.exp2(s - m_new)
        m_buf[rs, :] = m_new
        l_buf[rs, :] = l
        if g < draft:
            for i in range(ncol):
                s_ref[c0 + i, pl.ds(g, batch, stride=draft), :] = ss[i]

    def lhs(g, k):
        return x_buf[pl.ds(g * batch, batch), pl.ds(k * TILE, TILE)]

    def push(n, q, k):
        slot = lax.rem(n, RING)
        w = w_buf[slot, pl.ds(q * TILE, TILE), pl.ds(k * TILE, TILE)]
        pltpu.matmul_push_rhs(w, staging_register=k % 2, mxu_index=q, transpose=True)

    def mxu_body(*accs):
        acc = [[[accs[(a * 2 + q) * groups + g] for g in range(groups)] for q in range(2)] for a in range(2)]
        for a in range(2):
            for q in range(2):
                for g in range(groups):
                    pltpu.matmul_pop(acc[a][q][g])

        for copy in small:
            copy.wait()
        scale_buf[...] = jnp.broadcast_to(LOG2E / _row_to_col(temp_ref[...]), (batch, LANES))
        for g in range(draft + 1):
            h_copy(g).wait()
        for i in range(rows // 32):
            sl = pl.ds(i * 32, 32)
            h = h_buf[sl, :].astype(jnp.float32)
            r = lax.rsqrt(jnp.mean(h * h, axis=-1, keepdims=True) + 1e-5)
            x_buf[sl, :] = (h_buf[sl, :].astype(jnp.float32) * r * gain_ref[...]).astype(jnp.bfloat16)

        half = nk // 2

        def push_rest(q, kk):
            w = w_buf[full % RING, pl.ds(0, TILE), pl.ds((q * half + kk) * TILE, TILE)]
            pltpu.matmul_push_rhs(w, staging_register=kk % 2, mxu_index=q, transpose=True)

        def fullstep(n, a, issue, penalty=None, next_full=True):
            old = acc[1 - a]
            c_old = jnp.maximum(n - 1, 0) * (STEP // LANES)
            for k in range(nk):
                for q in range(2):
                    for g in range(groups):
                        pltpu.matmul_acc_lhs(acc[a][q][g], lhs(g, k), load_staged_rhs=k % 2 if g == 0 else None)
                for q in range(2):
                    if k + 1 < nk:
                        push(n, q, k + 1)
                    elif next_full:
                        push(n + 1, q, 0)
                    else:
                        push_rest(q, 0)
                if 1 <= k <= FENCES:
                    issue(k - 1)
                if k in SIG:
                    pl.semaphore_signal(fence, 1)
                for g in GRP.get(k, ()):
                    for q in range(2):
                        z = pltpu.matmul_pop(old[q][g])
                        online(g, q, c_old + q * (TILE // LANES), z, TILE // LANES,
                               None if penalty is None else [penalty] * (TILE // LANES))

            pl.semaphore_wait(fence, len(SIG))

        w_wait(0)
        for q in range(2):
            push(0, q, 0)

        split = (full - (RING - 1)) // 2 * 2
        tail = full // 2 * 2
        early = 1
        mid = nc - 1 - q_first - early * split
        assert mid >= 0 and tail == full - 1 and tokens >= TOK_STEP * full

        def issue_tokens(n):
            for i in range(TOK_STEP):
                token_copy(n * (TOK_STEP // draft) + i // draft, i % draft).start(priority=1)

        def issue_early(n, i):
            if i < W_PARTS:
                w_copy(n + RING - 1, i).start(priority=i % 2)
            elif i == W_PARTS:
                q_copy(q_first + n).start(priority=1)
            else:
                issue_tokens(n)

        def issue_late(n, i):
            if i == W_PARTS + 1:
                issue_tokens(n)

        @pl.loop(0, split // 2)
        def _(t):
            n = 2 * t
            w_wait(n + 1)
            fullstep(n, 0, lambda i: issue_early(n, i), penalty=jnp.where(t == 0, LOWEST, 0.0).astype(jnp.float32))
            w_wait(n + 2)
            fullstep(n + 1, 1, lambda i: issue_early(n + 1, i))

        for i, copy in enumerate(w_rest()):
            copy.start(priority=i % 2)

        @pl.loop(0, mid)
        def _(i):
            q_copy(q_first + early * split + i).start(priority=1)

        for i in range(TOK_STEP * full, tokens):
            token_copy(i // draft, i % draft).start(priority=1)

        @pl.loop(split // 2, tail // 2)
        def _(t):
            n = 2 * t
            w_wait(n + 1)
            fullstep(n, 0, lambda i: issue_late(n, i))
            w_wait(n + 2)
            fullstep(n + 1, 1, lambda i: issue_late(n + 1, i))

        n = full - 1
        for copy in w_rest():
            copy.wait()
        last_q().wait()
        for b in range(0, batch, 2):
            q_buf[nc - 1, pl.ds(b * draft, 2 * draft), pl.ds(0, last)] = jnp.concatenate([q_last[b], q_last[b + 1]], axis=0)
        fullstep(n, 0, lambda i: issue_late(n, i), next_full=False)
        for kk in range(half):
            for q in range(2):
                for g in range(groups):
                    pltpu.matmul_acc_lhs(acc[1][q][g], lhs(g, q * half + kk), load_staged_rhs=kk % 2 if g == 0 else None)
                if kk + 1 < half:
                    push_rest(q, kk + 1)
        for g in range(groups):
            for q in range(2):
                z = pltpu.matmul_pop(acc[0][q][g])
                online(g, q, n * (STEP // LANES) + q * (TILE // LANES), z, TILE // LANES)
        ncol = -(-rest // LANES)
        lane = lax.broadcasted_iota(jnp.int32, (batch, LANES), 1)
        pens = [None] * ncol
        for i in range(ncol):
            pens[i] = jnp.where(lane + i * LANES < rest, 0.0, LOWEST)
        for g in range(groups):
            z = pltpu.matmul_pop(acc[1][0][g]) + pltpu.matmul_pop(acc[1][1][g])
            online(g, 0, full * (STEP // LANES), z, ncol, pens)

    specs = [pltpu.ACC(q)((batch, TILE), jnp.float32) for a in range(2) for q in range(2) for g in range(groups)]
    pl.run_scoped(mxu_body, *specs)

    bulk = q_buf.at[pl.ds(q_first, nc - 1 - q_first)]
    pltpu.make_async_copy(bulk, bulk, q_sem.at[0]).wait()
    pltpu.make_async_copy(tile_ref, tile_ref, q_sem.at[2]).wait()


def _verify_kernel(
    dims,
    s_ref, q_in, m_ref, l_ref, tile_ref, tok_hbm, q_hbm,
    q_ref, col_buf, inv_ref, accept_ref, norm_ref, bonus_ref,
    gs_buf, part_buf, tok_smem, tok_ref,
    msg1, msg2, got1, got2,
    send1, recv1, send2, recv2, q_sem, tok_sem,
):
    del q_in
    batch, draft, vocab, ntp = dims
    nc = -(-vocab // LANES)
    last = vocab - (nc - 1) * LANES
    me = lax.axis_index("tp")
    barrier = pltpu.get_barrier_semaphore()
    for d in range(1, ntp):
        pl.semaphore_signal(barrier, inc=1, device_id={"tp": lax.rem(me + d, ntp)}, device_id_type=MESH)
    q_first = _q_first(vocab)
    qv = q_ref.reshape(nc, batch, draft, LANES)

    def q_copy(c):
        return pltpu.make_async_copy(
            q_hbm.at[:, :, pl.ds(pl.multiple_of(c * LANES, LANES), LANES)], qv.at[c], q_sem.at[c])

    tok_copies = [
        pltpu.make_async_copy(tok_hbm, tok_smem, tok_sem.at[0]),
        pltpu.make_async_copy(tok_hbm, tok_ref, tok_sem.at[1]),
    ]
    for copy in tok_copies:
        copy.start()

    @pl.loop(0, q_first)
    def _(c):
        q_copy(c).start()

    def remote(msg, got, send, recv, d):
        return pltpu.make_async_remote_copy(
            src_ref=msg, dst_ref=got.at[me], send_sem=send.at[d], recv_sem=recv.at[me],
            device_id={"tp": lax.rem(me + d, ntp)}, device_id_type=MESH)

    def arrived(msg, got, send, recv, d):
        src = lax.rem(me + d, ntp)
        return pltpu.make_async_remote_copy(
            src_ref=msg, dst_ref=got.at[src], send_sem=send.at[d], recv_sem=recv.at[src],
            device_id={"tp": src}, device_id_type=MESH)

    msg1[...] = jnp.zeros_like(msg1)
    for g in range(draft + 1):
        rs = pl.ds(g * batch, batch)
        m = m_ref[rs, :]
        top = jnp.max(m, axis=1, keepdims=True)
        tot = jnp.sum(l_ref[rs, :] * jnp.exp2(m - top), axis=1, keepdims=True)
        msg1[pl.ds(g, 1), pl.ds(0, batch)] = _col_to_row(top + jnp.log2(tot))

    def token_rows(src, dst):
        @pl.loop(0, batch, unroll=4)
        def _(b):
            for j in range(draft):
                idx = tok_smem[j, b] - me * vocab
                idx = jnp.minimum(jnp.maximum(idx, 0), vocab - 1)
                c = lax.shift_right_logical(idx, 7)
                dst[pl.ds(j * batch + b, 1), :] = src[c, pl.ds(b * draft + j, 1), :]

    pl.semaphore_wait(barrier, ntp - 1)
    for d in range(1, ntp):
        remote(msg1, got1, send1, recv1, d).start()
    got1[me] = msg1[...]

    for copy in tok_copies:
        copy.wait()
    token_rows(s_ref, gs_buf)
    msg2[...] = jnp.zeros_like(msg2)
    lane = lax.broadcasted_iota(jnp.int32, (batch, LANES), 1)
    for j in range(draft):
        idx = _row_to_col(tok_ref[pl.ds(j, 1), :].astype(jnp.float32)).astype(jnp.int32) - me * vocab
        owned = jnp.logical_and(idx >= 0, idx < vocab)
        hit = jnp.logical_and(owned, lane == jnp.bitwise_and(idx, LANES - 1))
        rs = pl.ds(j * batch, batch)
        tok_s = jnp.sum(jnp.where(hit, gs_buf[rs, :], 0.0), axis=1, keepdims=True)
        q_row = jnp.where(
            lax.shift_right_logical(idx, 7) == nc - 1,
            q_ref[nc - 1, pl.ds(j, batch, stride=draft), :],
            tile_ref[pl.ds((draft + 1) * j, batch, stride=draft * draft), :])
        tok_q = jnp.sum(jnp.where(hit, q_row, 0.0), axis=1, keepdims=True)
        msg2[pl.ds(draft + j, 1), pl.ds(0, batch)] = _col_to_row(tok_s)
        msg2[pl.ds(2 * draft + j, 1), pl.ds(0, batch)] = _col_to_row(tok_q)

    for d in range(1, ntp):
        arrived(msg1, got1, send1, recv1, d).wait_recv()
    top = got1[0]
    for i in range(1, ntp):
        top = jnp.maximum(top, got1[i])
    tot = jnp.exp2(got1[0] - top)
    for i in range(1, ntp):
        tot = tot + jnp.exp2(got1[i] - top)
    lse2 = top + jnp.log2(tot)
    bonus_ref[...] = lse2[draft:draft + 1, 0:batch] * LN2
    for j in range(draft):
        col_buf[pl.ds(j, batch, stride=draft), :] = jnp.broadcast_to(
            _row_to_col(lse2[j:j + 1, 0:batch]), (batch, LANES))

    @pl.loop(0, q_first)
    def _(c):
        q_copy(c).wait()

    last_mask = lax.broadcasted_iota(jnp.int32, (SLAB, LANES), 1) < last

    @pl.loop(0, batch * draft // SLAB)
    def _(v):
        rs = pl.ds(pl.multiple_of(v * SLAB, SLAB), SLAB)
        lse = col_buf[rs, :]

        def ex(c):
            return jnp.maximum(jnp.exp2(s_ref[c, rs, :] - lse) - q_ref[c, rs, :], 0.0)

        def chunk(t, total):
            for i in range(CHUNK):
                total = total + ex(t * CHUNK + i)
            return total

        part_buf[rs, :] = lax.fori_loop(
            0, (nc - 1) // CHUNK, chunk, jnp.where(last_mask, ex(nc - 1), 0.0))

    for j in range(draft):
        part = jnp.sum(part_buf[pl.ds(j, batch, stride=draft), :], axis=1, keepdims=True)
        msg2[pl.ds(j, 1), pl.ds(0, batch)] = _col_to_row(part)

    for d in range(1, ntp):
        remote(msg2, got2, send2, recv2, d).start()
    got2[me] = msg2[...]
    for d in range(1, ntp):
        arrived(msg2, got2, send2, recv2, d).wait_recv()
    tot = got2[0]
    for i in range(1, ntp):
        tot = tot + got2[i]
    norm = tot[0:draft, 0:batch]
    norm_ref[...] = norm
    target = jnp.exp2(tot[draft:2 * draft, 0:batch] - lse2[0:draft, 0:batch])
    accept_ref[...] = jnp.minimum(1.0, target / tot[2 * draft:3 * draft, 0:batch])
    for j in range(draft):
        inv_ref[pl.ds(j, batch, stride=draft), :] = jnp.broadcast_to(
            1.0 / _row_to_col(norm[j:j + 1, :]), (batch, LANES))
    for d in range(1, ntp):
        remote(msg1, got1, send1, recv1, d).wait_send()
        remote(msg2, got2, send2, recv2, d).wait_send()


OUT_GROUP = 5


def _write_kernel(
    dims, s_ref, q_ref, lse_ref, inv_ref, accept_in, norm_in, bonus_in,
    out_hbm, accept_ref, norm_ref, bonus_ref, stage, stage_last, sem,
):
    batch, draft, vocab = dims
    nc = -(-vocab // LANES)
    last = vocab - (nc - 1) * LANES
    view = stage.reshape(nc, batch, draft, LANES)
    ngroups = (nc - 1) // OUT_GROUP
    assert ngroups * OUT_GROUP == nc - 1

    def out_copy(c):
        return pltpu.make_async_copy(
            view.at[c], out_hbm.at[:, :, pl.ds(pl.multiple_of(c * LANES, LANES), LANES)], sem.at[0])

    def fill(c):
        stage[c] = jnp.maximum(jnp.exp2(s_ref[c] - lse_ref[...]) - q_ref[c], 0.0) * inv_ref[...]

    small = [
        pltpu.make_async_copy(src, dst, sem.at[2 + i])
        for i, (src, dst) in enumerate([(accept_in, accept_ref), (norm_in, norm_ref), (bonus_in, bonus_ref)])
    ]
    for copy in small:
        copy.start()
    fill(nc - 1)
    for b in range(batch):
        stage_last[b] = stage[nc - 1, pl.ds(b * draft, draft), pl.ds(0, last)]
    last_copy = pltpu.make_async_copy(stage_last, out_hbm.at[:, :, pl.ds((nc - 1) * LANES, last)], sem.at[1])
    last_copy.start()

    @pl.loop(0, ngroups)
    def _(t):
        for i in range(OUT_GROUP):
            fill(t * OUT_GROUP + i)
            out_copy(t * OUT_GROUP + i).start()

    last_copy.wait()
    for copy in small:
        copy.wait()
    bulk = stage.at[pl.ds(0, nc - 1)]
    pltpu.make_async_copy(bulk, bulk, sem.at[0]).wait()


def solution(mesh):
    ntp = mesh.shape["tp"]

    def local_step(hidden, norm_gain, w_head, draft_probs, draft_tokens, temperature):
        batch, draft, vocab = draft_probs.shape
        depth = hidden.shape[2]
        rows = batch * (draft + 1)
        nc = -(-vocab // LANES)
        vmem = pl.BlockSpec(memory_space=pltpu.VMEM)
        hbm = pl.BlockSpec(memory_space=pl.ANY)
        keep = functools.partial(pltpu.with_memory_space_constraint, memory_space=pltpu.VMEM)
        f32, bf16, dma = jnp.float32, jnp.bfloat16, pltpu.SemaphoreType.DMA
        vec = pltpu.VMEM((batch * draft, LANES), f32)
        big = pltpu.VMEM((nc, batch * draft, LANES), f32)
        stat = pltpu.VMEM((rows, LANES), f32)
        x = hidden.transpose(1, 0, 2).reshape(rows, depth)
        tok = draft_tokens.T
        s, q, m, l, tiles = pl.pallas_call(
            functools.partial(_logits_kernel, (batch, draft, depth, vocab)),
            out_shape=(big, big, stat, stat, pltpu.VMEM((batch * draft * draft, LANES), f32)),
            in_specs=[hbm] * 6,
            out_specs=(vmem,) * 5,
            scratch_shapes=[
                pltpu.VMEM((rows, depth), bf16),
                pltpu.VMEM((rows, depth), bf16),
                pltpu.VMEM((RING, STEP, depth), bf16),
                pltpu.VMEM((batch, draft, vocab - (nc - 1) * LANES), f32),
                pltpu.VMEM((batch, LANES), f32),
                pltpu.VMEM((1, depth), f32),
                pltpu.VMEM((1, batch), f32),
                pltpu.SMEM((draft, batch), jnp.int32),
                dma((draft + 1,)),
                dma((RING, W_PARTS)),
                dma((3,)),
                dma((3,)),
                pltpu.SemaphoreType.REGULAR,
            ],
            compiler_params=pltpu.CompilerParams(vmem_limit_bytes=GRANT),
            name="logits",
        )(x, norm_gain.reshape(1, depth), w_head.T, draft_probs, temperature.reshape(1, batch), tok)
        q, lse, inv, accept, norm, bonus = pl.pallas_call(
            functools.partial(_verify_kernel, (batch, draft, vocab, ntp)),
            out_shape=(
                big,
                vec,
                vec,
                pltpu.VMEM((draft, batch), f32),
                pltpu.VMEM((draft, batch), f32),
                pltpu.VMEM((1, batch), f32),
            ),
            in_specs=[vmem, vmem, vmem, vmem, vmem, hbm, hbm],
            out_specs=(vmem,) * 6,
            input_output_aliases={1: 0},
            scratch_shapes=[
                vec, vec,
                pltpu.SMEM((draft, batch), jnp.int32),
                pltpu.VMEM((draft, batch), jnp.int32),
                pltpu.VMEM((8, LANES), f32),
                pltpu.VMEM((16, LANES), f32),
                pltpu.VMEM((ntp, 8, LANES), f32),
                pltpu.VMEM((ntp, 16, LANES), f32),
                dma((ntp,)), dma((ntp,)), dma((ntp,)), dma((ntp,)), dma((nc,)), dma((2,)),
            ],
            compiler_params=pltpu.CompilerParams(
                collective_id=0, has_side_effects=True, vmem_limit_bytes=GRANT),
            name="verify",
        )(keep(s), keep(q), keep(m), keep(l), keep(tiles), tok, draft_probs)
        residual, accept, norm, bonus = pl.pallas_call(
            functools.partial(_write_kernel, (batch, draft, vocab)),
            out_shape=(
                jax.ShapeDtypeStruct(draft_probs.shape, f32),
                jax.ShapeDtypeStruct((draft, batch), f32),
                jax.ShapeDtypeStruct((draft, batch), f32),
                jax.ShapeDtypeStruct((1, batch), f32),
            ),
            in_specs=[vmem] * 7,
            out_specs=(hbm,) * 4,
            scratch_shapes=[
                big,
                pltpu.VMEM((batch, draft, vocab - (nc - 1) * LANES), f32),
                dma((5,)),
            ],
            compiler_params=pltpu.CompilerParams(vmem_limit_bytes=GRANT),
            name="write",
        )(*map(keep, (s, q, lse, inv, accept, norm, bonus)))
        return accept.T, norm.T, residual, bonus.reshape(batch)

    return jax.shard_map(
        local_step,
        mesh=mesh,
        in_specs=(P('dp', None, None), P(), P(None, 'tp'), P('dp', None, 'tp'), P('dp', None), P('dp')),
        out_specs=(P('dp', None), P('dp', None), P('dp', None, 'tp'), P('dp')),
        check_vma=False,
    )
```

```python
import functools

import jax
import jax.numpy as jnp
from jax import lax
from jax.experimental import pallas as pl
from jax.experimental.pallas import tpu as pltpu
from jax.sharding import PartitionSpec as P

LANES = 128
TILE = 256
STEP = 2 * TILE
RING = 10
SLAB = 64
CHUNK = 25
W_PARTS = 2
FENCES = 6
Q_LATE = 4
TOK_STEP = 8
SIG = (1, 3, 5, 7)
GRP = {1: (0,), 3: (1, 2), 5: (3, 4)}
GRANT = 26 * 1024 * 1024
LOG2E = 1.4426950408889634
LN2 = 0.6931471805599453
LOWEST = -3.4028234e38
MESH = pl.DeviceIdType.MESH


def _row_to_col(row):
    n = row.shape[1]
    r = lax.broadcasted_iota(jnp.int32, (n, n), 0)
    c = lax.broadcasted_iota(jnp.int32, (n, n), 1)
    return jnp.sum(jnp.where(r == c, row, 0.0), axis=1, keepdims=True)


def _col_to_row(col):
    n = col.shape[0]
    r = lax.broadcasted_iota(jnp.int32, (n, n), 0)
    c = lax.broadcasted_iota(jnp.int32, (n, n), 1)
    return jnp.sum(jnp.where(r == c, col, 0.0), axis=0, keepdims=True)


def _q_first(vocab):
    return (vocab // LANES) * Q_LATE // 8


def _logits_kernel(
    dims,
    x_hbm, gain_hbm, w_hbm, q_hbm, temp_hbm, tok_hbm,
    s_ref, q_buf, m_buf, l_buf, tile_ref,
    h_buf, x_buf, w_buf, q_last, scale_buf, gain_ref, temp_ref, tok_smem,
    h_sem, w_sem, q_sem, small_sem, fence,
):
    batch, draft, depth, vocab = dims
    tokens = batch * draft
    me = lax.axis_index("tp")
    q_first = _q_first(vocab)
    rows = batch * (draft + 1)
    nk = depth // TILE
    full = vocab // STEP
    rest = vocab - full * STEP
    nc = -(-vocab // LANES)
    last = vocab - (nc - 1) * LANES
    part = STEP // W_PARTS

    def w_copy(n, i, size=part):
        slot = lax.rem(n, RING)
        return pltpu.make_async_copy(
            w_hbm.at[pl.ds(n * STEP + i * part, size), :], w_buf.at[slot, pl.ds(i * part, size), :], w_sem.at[slot, i])

    def w_wait(n):
        for i in range(W_PARTS):
            w_copy(n, i).wait()

    def w_rest():
        return [w_copy(full, i, min(part, rest - i * part)) for i in range(-(-rest // part))]

    tiles = tile_ref.reshape(tokens, draft, LANES)
    qv = q_buf.reshape(nc, batch, draft, LANES)

    def q_copy(c):
        return pltpu.make_async_copy(
            q_hbm.at[:, :, pl.ds(pl.multiple_of(c * LANES, LANES), LANES)], qv.at[c], q_sem.at[0])

    def token_copy(b, j):
        idx = tok_smem[j, b] - me * vocab
        c = lax.shift_right_logical(jnp.minimum(jnp.maximum(idx, 0), vocab - 1), 7)
        c = jnp.minimum(c, nc - 2)
        return pltpu.make_async_copy(
            q_hbm.at[b, :, pl.ds(pl.multiple_of(c * LANES, LANES), LANES)], tiles.at[b * draft + j], q_sem.at[2])

    def last_q():
        return pltpu.make_async_copy(
            q_hbm.at[:, :, pl.ds((nc - 1) * LANES, last)], q_last, q_sem.at[1])

    def h_copy(g):
        rs = pl.ds(g * batch, batch)
        return pltpu.make_async_copy(x_hbm.at[rs, :], h_buf.at[rs, :], h_sem.at[g])

    small = [
        pltpu.make_async_copy(src, dst, small_sem.at[i])
        for i, (src, dst) in enumerate([(gain_hbm, gain_ref), (temp_hbm, temp_ref), (tok_hbm, tok_smem)])
    ]
    for g in range(draft + 1):
        h_copy(g).start()
    for copy in small:
        copy.start()
    for n in range(RING - 1):
        for i in range(W_PARTS):
            w_copy(n, i).start(priority=i % 2)
    last_q().start(priority=1)

    m_buf[...] = jnp.full_like(m_buf, LOWEST)
    l_buf[...] = jnp.zeros_like(l_buf)

    groups = draft + 1

    def online(g, q, c0, z, ncol, penalty=None):
        rs = pl.ds(g * batch, batch)
        scale = scale_buf[...]
        ss = [z[:, i * LANES:(i + 1) * LANES] * scale for i in range(ncol)]
        if penalty is not None:
            ss = [s + p for s, p in zip(ss, penalty)]
        m_old = m_buf[rs, :]
        m_new = m_old
        for s in ss:
            m_new = jnp.maximum(m_new, s)
        l = l_buf[rs, :] * jnp.exp2(m_old - m_new)
        for s in ss:
            l = l + jnp.exp2(s - m_new)
        m_buf[rs, :] = m_new
        l_buf[rs, :] = l
        if g < draft:
            for i in range(ncol):
                s_ref[c0 + i, pl.ds(g, batch, stride=draft), :] = ss[i]

    def lhs(g, k):
        return x_buf[pl.ds(g * batch, batch), pl.ds(k * TILE, TILE)]

    def push(n, q, k):
        slot = lax.rem(n, RING)
        w = w_buf[slot, pl.ds(q * TILE, TILE), pl.ds(k * TILE, TILE)]
        pltpu.matmul_push_rhs(w, staging_register=k % 2, mxu_index=q, transpose=True)

    def mxu_body(*accs):
        acc = [[[accs[(a * 2 + q) * groups + g] for g in range(groups)] for q in range(2)] for a in range(2)]
        for a in range(2):
            for q in range(2):
                for g in range(groups):
                    pltpu.matmul_pop(acc[a][q][g])

        for copy in small:
            copy.wait()
        scale_buf[...] = jnp.broadcast_to(LOG2E / _row_to_col(temp_ref[...]), (batch, LANES))
        for g in range(draft + 1):
            h_copy(g).wait()
        for i in range(rows // 32):
            sl = pl.ds(i * 32, 32)
            h = h_buf[sl, :].astype(jnp.float32)
            r = lax.rsqrt(jnp.mean(h * h, axis=-1, keepdims=True) + 1e-5)
            x_buf[sl, :] = (h_buf[sl, :].astype(jnp.float32) * r * gain_ref[...]).astype(jnp.bfloat16)

        half = nk // 2

        def push_rest(q, kk):
            w = w_buf[full % RING, pl.ds(0, TILE), pl.ds((q * half + kk) * TILE, TILE)]
            pltpu.matmul_push_rhs(w, staging_register=kk % 2, mxu_index=q, transpose=True)

        def fullstep(n, a, issue, penalty=None, next_full=True):
            old = acc[1 - a]
            c_old = jnp.maximum(n - 1, 0) * (STEP // LANES)
            for k in range(nk):
                for q in range(2):
                    for g in range(groups):
                        pltpu.matmul_acc_lhs(acc[a][q][g], lhs(g, k), load_staged_rhs=k % 2 if g == 0 else None)
                for q in range(2):
                    if k + 1 < nk:
                        push(n, q, k + 1)
                    elif next_full:
                        push(n + 1, q, 0)
                    else:
                        push_rest(q, 0)
                if 1 <= k <= FENCES:
                    issue(k - 1)
                if k in SIG:
                    pl.semaphore_signal(fence, 1)
                for g in GRP.get(k, ()):
                    for q in range(2):
                        z = pltpu.matmul_pop(old[q][g])
                        online(g, q, c_old + q * (TILE // LANES), z, TILE // LANES,
                               None if penalty is None else [penalty] * (TILE // LANES))

            pl.semaphore_wait(fence, len(SIG))

        w_wait(0)
        for q in range(2):
            push(0, q, 0)

        split = (full - (RING - 1)) // 2 * 2
        tail = full // 2 * 2
        early = 1
        mid = nc - 1 - q_first - early * split
        assert mid >= 0 and tail == full - 1 and tokens >= TOK_STEP * full

        def issue_tokens(n):
            for i in range(TOK_STEP):
                token_copy(n * (TOK_STEP // draft) + i // draft, i % draft).start(priority=1)

        def issue_early(n, i):
            if i < W_PARTS:
                w_copy(n + RING - 1, i).start(priority=i % 2)
            elif i == W_PARTS:
                q_copy(q_first + n).start(priority=1)
            elif i == W_PARTS + 1:
                issue_tokens(n)

        def issue_late(n, i):
            if i == W_PARTS + 1:
                issue_tokens(n)

        @pl.loop(0, split // 2)
        def _(t):
            n = 2 * t
            w_wait(n + 1)
            fullstep(n, 0, lambda i: issue_early(n, i), penalty=jnp.where(t == 0, LOWEST, 0.0).astype(jnp.float32))
            w_wait(n + 2)
            fullstep(n + 1, 1, lambda i: issue_early(n + 1, i))

        for i, copy in enumerate(w_rest()):
            copy.start(priority=i % 2)

        @pl.loop(0, mid)
        def _(i):
            q_copy(q_first + early * split + i).start(priority=1)

        for i in range(TOK_STEP * full, tokens):
            token_copy(i // draft, i % draft).start(priority=1)

        @pl.loop(split // 2, tail // 2)
        def _(t):
            n = 2 * t
            w_wait(n + 1)
            fullstep(n, 0, lambda i: issue_late(n, i))
            w_wait(n + 2)
            fullstep(n + 1, 1, lambda i: issue_late(n + 1, i))

        n = full - 1
        for copy in w_rest():
            copy.wait()
        last_q().wait()
        for b in range(0, batch, 2):
            q_buf[nc - 1, pl.ds(b * draft, 2 * draft), pl.ds(0, last)] = jnp.concatenate([q_last[b], q_last[b + 1]], axis=0)
        fullstep(n, 0, lambda i: issue_late(n, i), next_full=False)
        for kk in range(half):
            for q in range(2):
                for g in range(groups):
                    pltpu.matmul_acc_lhs(acc[1][q][g], lhs(g, q * half + kk), load_staged_rhs=kk % 2 if g == 0 else None)
                if kk + 1 < half:
                    push_rest(q, kk + 1)
        for g in range(groups):
            for q in range(2):
                z = pltpu.matmul_pop(acc[0][q][g])
                online(g, q, n * (STEP // LANES) + q * (TILE // LANES), z, TILE // LANES)
        ncol = -(-rest // LANES)
        lane = lax.broadcasted_iota(jnp.int32, (batch, LANES), 1)
        pens = [None] * ncol
        for i in range(ncol):
            pens[i] = jnp.where(lane + i * LANES < rest, 0.0, LOWEST)
        for g in range(groups):
            z = pltpu.matmul_pop(acc[1][0][g]) + pltpu.matmul_pop(acc[1][1][g])
            online(g, 0, full * (STEP // LANES), z, ncol, pens)

    specs = [pltpu.ACC(q)((batch, TILE), jnp.float32) for a in range(2) for q in range(2) for g in range(groups)]
    pl.run_scoped(mxu_body, *specs)

    bulk = q_buf.at[pl.ds(q_first, nc - 1 - q_first)]
    pltpu.make_async_copy(bulk, bulk, q_sem.at[0]).wait()
    pltpu.make_async_copy(tile_ref, tile_ref, q_sem.at[2]).wait()


def _verify_kernel(
    dims,
    s_ref, q_in, m_ref, l_ref, tile_ref, tok_hbm, q_hbm,
    q_ref, col_buf, inv_ref, accept_ref, norm_ref, bonus_ref,
    gs_buf, part_buf, tok_smem, tok_ref,
    msg1, msg2, got1, got2,
    send1, recv1, send2, recv2, q_sem, tok_sem,
):
    del q_in
    batch, draft, vocab, ntp = dims
    nc = -(-vocab // LANES)
    last = vocab - (nc - 1) * LANES
    me = lax.axis_index("tp")
    barrier = pltpu.get_barrier_semaphore()
    for d in range(1, ntp):
        pl.semaphore_signal(barrier, inc=1, device_id={"tp": lax.rem(me + d, ntp)}, device_id_type=MESH)
    q_first = _q_first(vocab)
    qv = q_ref.reshape(nc, batch, draft, LANES)

    def q_copy(c):
        return pltpu.make_async_copy(
            q_hbm.at[:, :, pl.ds(pl.multiple_of(c * LANES, LANES), LANES)], qv.at[c], q_sem.at[c])

    tok_copies = [
        pltpu.make_async_copy(tok_hbm, tok_smem, tok_sem.at[0]),
        pltpu.make_async_copy(tok_hbm, tok_ref, tok_sem.at[1]),
    ]
    for copy in tok_copies:
        copy.start()

    def remote(msg, got, send, recv, d):
        return pltpu.make_async_remote_copy(
            src_ref=msg, dst_ref=got.at[me], send_sem=send.at[d], recv_sem=recv.at[me],
            device_id={"tp": lax.rem(me + d, ntp)}, device_id_type=MESH)

    def arrived(msg, got, send, recv, d):
        src = lax.rem(me + d, ntp)
        return pltpu.make_async_remote_copy(
            src_ref=msg, dst_ref=got.at[src], send_sem=send.at[d], recv_sem=recv.at[src],
            device_id={"tp": src}, device_id_type=MESH)

    msg1[...] = jnp.zeros_like(msg1)
    for g in range(draft + 1):
        rs = pl.ds(g * batch, batch)
        m = m_ref[rs, :]
        top = jnp.max(m, axis=1, keepdims=True)
        tot = jnp.sum(l_ref[rs, :] * jnp.exp2(m - top), axis=1, keepdims=True)
        msg1[pl.ds(g, 1), pl.ds(0, batch)] = _col_to_row(top + jnp.log2(tot))

    def token_rows(src, dst):
        @pl.loop(0, batch, unroll=8)
        def _(b):
            for j in range(draft):
                idx = tok_smem[j, b] - me * vocab
                idx = jnp.minimum(jnp.maximum(idx, 0), vocab - 1)
                c = lax.shift_right_logical(idx, 7)
                dst[pl.ds(j * batch + b, 1), :] = src[c, pl.ds(b * draft + j, 1), :]

    pl.semaphore_wait(barrier, ntp - 1)
    for d in range(1, ntp):
        remote(msg1, got1, send1, recv1, d).start()
    got1[me] = msg1[...]

    @pl.loop(0, q_first)
    def _(c):
        q_copy(c).start()

    for copy in tok_copies:
        copy.wait()
    token_rows(s_ref, gs_buf)
    msg2[...] = jnp.zeros_like(msg2)
    lane = lax.broadcasted_iota(jnp.int32, (batch, LANES), 1)
    for j in range(draft):
        idx = _row_to_col(tok_ref[pl.ds(j, 1), :].astype(jnp.float32)).astype(jnp.int32) - me * vocab
        owned = jnp.logical_and(idx >= 0, idx < vocab)
        hit = jnp.logical_and(owned, lane == jnp.bitwise_and(idx, LANES - 1))
        rs = pl.ds(j * batch, batch)
        tok_s = jnp.sum(jnp.where(hit, gs_buf[rs, :], 0.0), axis=1, keepdims=True)
        q_row = jnp.where(
            lax.shift_right_logical(idx, 7) == nc - 1,
            q_ref[nc - 1, pl.ds(j, batch, stride=draft), :],
            tile_ref[pl.ds((draft + 1) * j, batch, stride=draft * draft), :])
        tok_q = jnp.sum(jnp.where(hit, q_row, 0.0), axis=1, keepdims=True)
        msg2[pl.ds(draft + j, 1), pl.ds(0, batch)] = _col_to_row(tok_s)
        msg2[pl.ds(2 * draft + j, 1), pl.ds(0, batch)] = _col_to_row(tok_q)

    for d in range(1, ntp):
        arrived(msg1, got1, send1, recv1, d).wait_recv()
    top = got1[0]
    for i in range(1, ntp):
        top = jnp.maximum(top, got1[i])
    tot = jnp.exp2(got1[0] - top)
    for i in range(1, ntp):
        tot = tot + jnp.exp2(got1[i] - top)
    lse2 = top + jnp.log2(tot)
    bonus_ref[...] = lse2[draft:draft + 1, 0:batch] * LN2
    for j in range(draft):
        col_buf[pl.ds(j, batch, stride=draft), :] = jnp.broadcast_to(
            _row_to_col(lse2[j:j + 1, 0:batch]), (batch, LANES))

    @pl.loop(0, q_first)
    def _(c):
        q_copy(c).wait()

    last_mask = lax.broadcasted_iota(jnp.int32, (SLAB, LANES), 1) < last

    @pl.loop(0, batch * draft // SLAB)
    def _(v):
        rs = pl.ds(pl.multiple_of(v * SLAB, SLAB), SLAB)
        lse = col_buf[rs, :]

        def ex(c):
            return jnp.maximum(jnp.exp2(s_ref[c, rs, :] - lse) - q_ref[c, rs, :], 0.0)

        def chunk(t, total):
            for i in range(CHUNK):
                total = total + ex(t * CHUNK + i)
            return total

        part_buf[rs, :] = lax.fori_loop(
            0, (nc - 1) // CHUNK, chunk, jnp.where(last_mask, ex(nc - 1), 0.0))

    for j in range(draft):
        part = jnp.sum(part_buf[pl.ds(j, batch, stride=draft), :], axis=1, keepdims=True)
        msg2[pl.ds(j, 1), pl.ds(0, batch)] = _col_to_row(part)

    for d in range(1, ntp):
        remote(msg2, got2, send2, recv2, d).start()
    got2[me] = msg2[...]
    for d in range(1, ntp):
        arrived(msg2, got2, send2, recv2, d).wait_recv()
    tot = got2[0]
    for i in range(1, ntp):
        tot = tot + got2[i]
    norm = tot[0:draft, 0:batch]
    norm_ref[...] = norm
    target = jnp.exp2(tot[draft:2 * draft, 0:batch] - lse2[0:draft, 0:batch])
    accept_ref[...] = jnp.minimum(1.0, target / tot[2 * draft:3 * draft, 0:batch])
    for j in range(draft):
        inv_ref[pl.ds(j, batch, stride=draft), :] = jnp.broadcast_to(
            1.0 / _row_to_col(norm[j:j + 1, :]), (batch, LANES))
    for d in range(1, ntp):
        remote(msg1, got1, send1, recv1, d).wait_send()
        remote(msg2, got2, send2, recv2, d).wait_send()


OUT_GROUP = 5


def _write_kernel(
    dims, s_ref, q_ref, lse_ref, inv_ref, accept_in, norm_in, bonus_in,
    out_hbm, accept_ref, norm_ref, bonus_ref, stage, stage_last, sem,
):
    batch, draft, vocab = dims
    nc = -(-vocab // LANES)
    last = vocab - (nc - 1) * LANES
    view = stage.reshape(nc, batch, draft, LANES)
    ngroups = (nc - 1) // OUT_GROUP
    assert ngroups * OUT_GROUP == nc - 1

    def out_copy(c):
        return pltpu.make_async_copy(
            view.at[c], out_hbm.at[:, :, pl.ds(pl.multiple_of(c * LANES, LANES), LANES)], sem.at[0])

    def fill(c):
        stage[c] = jnp.maximum(jnp.exp2(s_ref[c] - lse_ref[...]) - q_ref[c], 0.0) * inv_ref[...]

    small = [
        pltpu.make_async_copy(src, dst, sem.at[2 + i])
        for i, (src, dst) in enumerate([(accept_in, accept_ref), (norm_in, norm_ref), (bonus_in, bonus_ref)])
    ]
    for copy in small:
        copy.start()
    fill(nc - 1)
    for b in range(batch):
        stage_last[b] = stage[nc - 1, pl.ds(b * draft, draft), pl.ds(0, last)]
    last_copy = pltpu.make_async_copy(stage_last, out_hbm.at[:, :, pl.ds((nc - 1) * LANES, last)], sem.at[1])
    last_copy.start()

    @pl.loop(0, ngroups)
    def _(t):
        for i in range(OUT_GROUP):
            fill(t * OUT_GROUP + i)
            out_copy(t * OUT_GROUP + i).start()

    last_copy.wait()
    for copy in small:
        copy.wait()
    bulk = stage.at[pl.ds(0, nc - 1)]
    pltpu.make_async_copy(bulk, bulk, sem.at[0]).wait()


def solution(mesh):
    ntp = mesh.shape["tp"]

    def local_step(hidden, norm_gain, w_head, draft_probs, draft_tokens, temperature):
        batch, draft, vocab = draft_probs.shape
        depth = hidden.shape[2]
        rows = batch * (draft + 1)
        nc = -(-vocab // LANES)
        vmem = pl.BlockSpec(memory_space=pltpu.VMEM)
        hbm = pl.BlockSpec(memory_space=pl.ANY)
        keep = functools.partial(pltpu.with_memory_space_constraint, memory_space=pltpu.VMEM)
        f32, bf16, dma = jnp.float32, jnp.bfloat16, pltpu.SemaphoreType.DMA
        vec = pltpu.VMEM((batch * draft, LANES), f32)
        big = pltpu.VMEM((nc, batch * draft, LANES), f32)
        stat = pltpu.VMEM((rows, LANES), f32)
        x = hidden.transpose(1, 0, 2).reshape(rows, depth)
        tok = draft_tokens.T
        s, q, m, l, tiles = pl.pallas_call(
            functools.partial(_logits_kernel, (batch, draft, depth, vocab)),
            out_shape=(big, big, stat, stat, pltpu.VMEM((batch * draft * draft, LANES), f32)),
            in_specs=[hbm] * 6,
            out_specs=(vmem,) * 5,
            scratch_shapes=[
                pltpu.VMEM((rows, depth), bf16),
                pltpu.VMEM((rows, depth), bf16),
                pltpu.VMEM((RING, STEP, depth), bf16),
                pltpu.VMEM((batch, draft, vocab - (nc - 1) * LANES), f32),
                pltpu.VMEM((batch, LANES), f32),
                pltpu.VMEM((1, depth), f32),
                pltpu.VMEM((1, batch), f32),
                pltpu.SMEM((draft, batch), jnp.int32),
                dma((draft + 1,)),
                dma((RING, W_PARTS)),
                dma((3,)),
                dma((3,)),
                pltpu.SemaphoreType.REGULAR,
            ],
            compiler_params=pltpu.CompilerParams(vmem_limit_bytes=GRANT),
            name="logits",
        )(x, norm_gain.reshape(1, depth), w_head.T, draft_probs, temperature.reshape(1, batch), tok)
        q, lse, inv, accept, norm, bonus = pl.pallas_call(
            functools.partial(_verify_kernel, (batch, draft, vocab, ntp)),
            out_shape=(
                big,
                vec,
                vec,
                pltpu.VMEM((draft, batch), f32),
                pltpu.VMEM((draft, batch), f32),
                pltpu.VMEM((1, batch), f32),
            ),
            in_specs=[vmem, vmem, vmem, vmem, vmem, hbm, hbm],
            out_specs=(vmem,) * 6,
            input_output_aliases={1: 0},
            scratch_shapes=[
                vec, vec,
                pltpu.SMEM((draft, batch), jnp.int32),
                pltpu.VMEM((draft, batch), jnp.int32),
                pltpu.VMEM((8, LANES), f32),
                pltpu.VMEM((16, LANES), f32),
                pltpu.VMEM((ntp, 8, LANES), f32),
                pltpu.VMEM((ntp, 16, LANES), f32),
                dma((ntp,)), dma((ntp,)), dma((ntp,)), dma((ntp,)), dma((nc,)), dma((2,)),
            ],
            compiler_params=pltpu.CompilerParams(
                collective_id=0, has_side_effects=True, vmem_limit_bytes=GRANT),
            name="verify",
        )(keep(s), keep(q), keep(m), keep(l), keep(tiles), tok, draft_probs)
        residual, accept, norm, bonus = pl.pallas_call(
            functools.partial(_write_kernel, (batch, draft, vocab)),
            out_shape=(
                jax.ShapeDtypeStruct(draft_probs.shape, f32),
                jax.ShapeDtypeStruct((draft, batch), f32),
                jax.ShapeDtypeStruct((draft, batch), f32),
                jax.ShapeDtypeStruct((1, batch), f32),
            ),
            in_specs=[vmem] * 7,
            out_specs=(hbm,) * 4,
            scratch_shapes=[
                big,
                pltpu.VMEM((batch, draft, vocab - (nc - 1) * LANES), f32),
                dma((5,)),
            ],
            compiler_params=pltpu.CompilerParams(vmem_limit_bytes=GRANT),
            name="write",
        )(*map(keep, (s, q, lse, inv, accept, norm, bonus)))
        return accept.T, norm.T, residual, bonus.reshape(batch)

    return jax.shard_map(
        local_step,
        mesh=mesh,
        in_specs=(P('dp', None, None), P(), P(None, 'tp'), P('dp', None, 'tp'), P('dp', None), P('dp')),
        out_specs=(P('dp', None), P('dp', None), P('dp', None, 'tp'), P('dp')),
        check_vma=False,
    )
```

```python
import functools

import jax
import jax.numpy as jnp
from jax import lax
from jax.experimental import pallas as pl
from jax.experimental.pallas import tpu as pltpu
from jax.sharding import PartitionSpec as P

LANES = 128
TILE = 256
STEP = 2 * TILE
RING = 10
SLAB = 64
CHUNK = 25
W_PARTS = 2
FENCES = 6
Q_LATE = 4
TOK_STEP = 8
SIG = (1, 3, 5, 7)
GRP = {1: (0,), 3: (1, 2), 5: (3, 4)}
GRANT = 26 * 1024 * 1024
LOG2E = 1.4426950408889634
LN2 = 0.6931471805599453
LOWEST = -3.4028234e38
MESH = pl.DeviceIdType.MESH


def _row_to_col(row):
    n = row.shape[1]
    r = lax.broadcasted_iota(jnp.int32, (n, n), 0)
    c = lax.broadcasted_iota(jnp.int32, (n, n), 1)
    return jnp.sum(jnp.where(r == c, row, 0.0), axis=1, keepdims=True)


def _col_to_row(col):
    n = col.shape[0]
    r = lax.broadcasted_iota(jnp.int32, (n, n), 0)
    c = lax.broadcasted_iota(jnp.int32, (n, n), 1)
    return jnp.sum(jnp.where(r == c, col, 0.0), axis=0, keepdims=True)


def _q_first(vocab):
    return (vocab // LANES) * Q_LATE // 8


def _logits_kernel(
    dims,
    x_hbm, gain_hbm, w_hbm, q_hbm, temp_hbm, tok_hbm,
    s_ref, q_buf, m_buf, l_buf, tile_ref,
    h_buf, x_buf, w_buf, q_last, scale_buf, gain_ref, temp_ref, tok_smem,
    h_sem, w_sem, q_sem, small_sem, fence,
):
    batch, draft, depth, vocab = dims
    tokens = batch * draft
    me = lax.axis_index("tp")
    q_first = _q_first(vocab)
    rows = batch * (draft + 1)
    nk = depth // TILE
    full = vocab // STEP
    rest = vocab - full * STEP
    nc = -(-vocab // LANES)
    last = vocab - (nc - 1) * LANES
    part = STEP // W_PARTS

    def w_copy(n, i, size=part):
        slot = lax.rem(n, RING)
        return pltpu.make_async_copy(
            w_hbm.at[pl.ds(n * STEP + i * part, size), :], w_buf.at[slot, pl.ds(i * part, size), :], w_sem.at[slot, i])

    def w_wait(n):
        for i in range(W_PARTS):
            w_copy(n, i).wait()

    def w_rest():
        return [w_copy(full, i, min(part, rest - i * part)) for i in range(-(-rest // part))]

    tiles = tile_ref.reshape(tokens, draft, LANES)
    qv = q_buf.reshape(nc, batch, draft, LANES)

    def q_copy(c):
        return pltpu.make_async_copy(
            q_hbm.at[:, :, pl.ds(pl.multiple_of(c * LANES, LANES), LANES)], qv.at[c], q_sem.at[0])

    def token_copy(b, j):
        idx = tok_smem[j, b] - me * vocab
        c = lax.shift_right_logical(jnp.minimum(jnp.maximum(idx, 0), vocab - 1), 7)
        c = jnp.minimum(c, nc - 2)
        return pltpu.make_async_copy(
            q_hbm.at[b, :, pl.ds(pl.multiple_of(c * LANES, LANES), LANES)], tiles.at[b * draft + j], q_sem.at[2])

    def last_q():
        return pltpu.make_async_copy(
            q_hbm.at[:, :, pl.ds((nc - 1) * LANES, last)], q_last, q_sem.at[1])

    def h_copy(g):
        rs = pl.ds(g * batch, batch)
        return pltpu.make_async_copy(x_hbm.at[rs, :], h_buf.at[rs, :], h_sem)

    small = [
        pltpu.make_async_copy(src, dst, small_sem.at[i])
        for i, (src, dst) in enumerate([(gain_hbm, gain_ref), (temp_hbm, temp_ref), (tok_hbm, tok_smem)])
    ]
    for g in range(draft + 1):
        h_copy(g).start()
    for copy in small:
        copy.start()
    for n in range(RING - 1):
        for i in range(W_PARTS):
            w_copy(n, i).start(priority=i % 2)
    last_q().start(priority=1)

    m_buf[...] = jnp.full_like(m_buf, LOWEST)
    l_buf[...] = jnp.zeros_like(l_buf)

    groups = draft + 1

    def online(g, q, c0, z, ncol, penalty=None):
        rs = pl.ds(g * batch, batch)
        scale = scale_buf[...]
        ss = [z[:, i * LANES:(i + 1) * LANES] * scale for i in range(ncol)]
        if penalty is not None:
            ss = [s + p for s, p in zip(ss, penalty)]
        m_old = m_buf[rs, :]
        m_new = m_old
        for s in ss:
            m_new = jnp.maximum(m_new, s)
        l = l_buf[rs, :] * jnp.exp2(m_old - m_new)
        for s in ss:
            l = l + jnp.exp2(s - m_new)
        m_buf[rs, :] = m_new
        l_buf[rs, :] = l
        if g < draft:
            for i in range(ncol):
                s_ref[c0 + i, pl.ds(g, batch, stride=draft), :] = ss[i]

    def lhs(g, k):
        return x_buf[pl.ds(g * batch, batch), pl.ds(k * TILE, TILE)]

    def push(n, q, k):
        slot = lax.rem(n, RING)
        w = w_buf[slot, pl.ds(q * TILE, TILE), pl.ds(k * TILE, TILE)]
        pltpu.matmul_push_rhs(w, staging_register=k % 2, mxu_index=q, transpose=True)

    def mxu_body(*accs):
        acc = [[[accs[(a * 2 + q) * groups + g] for g in range(groups)] for q in range(2)] for a in range(2)]
        for a in range(2):
            for q in range(2):
                for g in range(groups):
                    pltpu.matmul_pop(acc[a][q][g])

        for copy in small:
            copy.wait()
        scale_buf[...] = jnp.broadcast_to(LOG2E / _row_to_col(temp_ref[...]), (batch, LANES))
        for g in range(draft + 1):
            h_copy(g).wait()
        for i in range(rows // 32):
            sl = pl.ds(i * 32, 32)
            h = h_buf[sl, :].astype(jnp.float32)
            r = lax.rsqrt(jnp.mean(h * h, axis=-1, keepdims=True) + 1e-5)
            x_buf[sl, :] = (h_buf[sl, :].astype(jnp.float32) * r * gain_ref[...]).astype(jnp.bfloat16)

        half = nk // 2

        def push_rest(q, kk):
            w = w_buf[full % RING, pl.ds(0, TILE), pl.ds((q * half + kk) * TILE, TILE)]
            pltpu.matmul_push_rhs(w, staging_register=kk % 2, mxu_index=q, transpose=True)

        def fullstep(n, a, issue, penalty=None, next_full=True):
            old = acc[1 - a]
            c_old = jnp.maximum(n - 1, 0) * (STEP // LANES)
            for k in range(nk):
                for q in range(2):
                    for g in range(groups):
                        pltpu.matmul_acc_lhs(acc[a][q][g], lhs(g, k), load_staged_rhs=k % 2 if g == 0 else None)
                for q in range(2):
                    if k + 1 < nk:
                        push(n, q, k + 1)
                    elif next_full:
                        push(n + 1, q, 0)
                    else:
                        push_rest(q, 0)
                if 1 <= k <= FENCES:
                    issue(k - 1)
                if k in SIG:
                    pl.semaphore_signal(fence, 1)
                for g in GRP.get(k, ()):
                    for q in range(2):
                        z = pltpu.matmul_pop(old[q][g])
                        online(g, q, c_old + q * (TILE // LANES), z, TILE // LANES,
                               None if penalty is None else [penalty] * (TILE // LANES))

            pl.semaphore_wait(fence, len(SIG))

        w_wait(0)
        for q in range(2):
            push(0, q, 0)

        split = (full - (RING - 1)) // 2 * 2
        tail = full // 2 * 2
        early = 1
        mid = nc - 1 - q_first - early * split
        assert mid >= 0 and tail == full - 1 and tokens >= TOK_STEP * full

        def issue_tokens(n):
            for i in range(TOK_STEP):
                token_copy(n * (TOK_STEP // draft) + i // draft, i % draft).start(priority=1)

        def issue_early(n, i):
            if i < W_PARTS:
                w_copy(n + RING - 1, i).start(priority=i % 2)
            elif i == W_PARTS:
                q_copy(q_first + n).start(priority=1)
            elif i == W_PARTS + 1:
                issue_tokens(n)

        def issue_late(n, i):
            if i == W_PARTS + 1:
                issue_tokens(n)

        @pl.loop(0, split // 2)
        def _(t):
            n = 2 * t
            w_wait(n + 1)
            fullstep(n, 0, lambda i: issue_early(n, i), penalty=jnp.where(t == 0, LOWEST, 0.0).astype(jnp.float32))
            w_wait(n + 2)
            fullstep(n + 1, 1, lambda i: issue_early(n + 1, i))

        for i, copy in enumerate(w_rest()):
            copy.start(priority=i % 2)

        @pl.loop(0, mid)
        def _(i):
            q_copy(q_first + early * split + i).start(priority=1)

        for i in range(TOK_STEP * full, tokens):
            token_copy(i // draft, i % draft).start(priority=1)

        @pl.loop(split // 2, tail // 2)
        def _(t):
            n = 2 * t
            w_wait(n + 1)
            fullstep(n, 0, lambda i: issue_late(n, i))
            w_wait(n + 2)
            fullstep(n + 1, 1, lambda i: issue_late(n + 1, i))

        n = full - 1
        for copy in w_rest():
            copy.wait()
        last_q().wait()
        for b in range(0, batch, 2):
            q_buf[nc - 1, pl.ds(b * draft, 2 * draft), pl.ds(0, last)] = jnp.concatenate([q_last[b], q_last[b + 1]], axis=0)
        fullstep(n, 0, lambda i: issue_late(n, i), next_full=False)
        for kk in range(half):
            for q in range(2):
                for g in range(groups):
                    pltpu.matmul_acc_lhs(acc[1][q][g], lhs(g, q * half + kk), load_staged_rhs=kk % 2 if g == 0 else None)
                if kk + 1 < half:
                    push_rest(q, kk + 1)
        for g in range(groups):
            for q in range(2):
                z = pltpu.matmul_pop(acc[0][q][g])
                online(g, q, n * (STEP // LANES) + q * (TILE // LANES), z, TILE // LANES)
        ncol = -(-rest // LANES)
        lane = lax.broadcasted_iota(jnp.int32, (batch, LANES), 1)
        pens = [None] * ncol
        for i in range(ncol):
            pens[i] = jnp.where(lane + i * LANES < rest, 0.0, LOWEST)
        for g in range(groups):
            z = pltpu.matmul_pop(acc[1][0][g]) + pltpu.matmul_pop(acc[1][1][g])
            online(g, 0, full * (STEP // LANES), z, ncol, pens)

    specs = [pltpu.ACC(q)((batch, TILE), jnp.float32) for a in range(2) for q in range(2) for g in range(groups)]
    pl.run_scoped(mxu_body, *specs)

    bulk = q_buf.at[pl.ds(q_first, nc - 1 - q_first)]
    pltpu.make_async_copy(bulk, bulk, q_sem.at[0]).wait()
    pltpu.make_async_copy(tile_ref, tile_ref, q_sem.at[2]).wait()


def _verify_kernel(
    dims,
    s_ref, q_in, m_ref, l_ref, tile_ref, tok_hbm, q_hbm,
    q_ref, col_buf, inv_ref, accept_ref, norm_ref, bonus_ref,
    gs_buf, part_buf, tok_smem, tok_ref,
    msg1, msg2, got1, got2,
    send1, recv1, send2, recv2, q_sem, tok_sem,
):
    del q_in
    batch, draft, vocab, ntp = dims
    nc = -(-vocab // LANES)
    last = vocab - (nc - 1) * LANES
    me = lax.axis_index("tp")
    barrier = pltpu.get_barrier_semaphore()
    for d in range(1, ntp):
        pl.semaphore_signal(barrier, inc=1, device_id={"tp": lax.rem(me + d, ntp)}, device_id_type=MESH)
    q_first = _q_first(vocab)
    qv = q_ref.reshape(nc, batch, draft, LANES)

    def q_copy(c):
        return pltpu.make_async_copy(
            q_hbm.at[:, :, pl.ds(pl.multiple_of(c * LANES, LANES), LANES)], qv.at[c], q_sem)

    tok_copies = [
        pltpu.make_async_copy(tok_hbm, tok_smem, tok_sem.at[0]),
        pltpu.make_async_copy(tok_hbm, tok_ref, tok_sem.at[1]),
    ]
    for copy in tok_copies:
        copy.start()

    def remote(msg, got, send, recv, d):
        return pltpu.make_async_remote_copy(
            src_ref=msg, dst_ref=got.at[me], send_sem=send.at[d], recv_sem=recv.at[me],
            device_id={"tp": lax.rem(me + d, ntp)}, device_id_type=MESH)

    def arrived(msg, got, send, recv, d):
        src = lax.rem(me + d, ntp)
        return pltpu.make_async_remote_copy(
            src_ref=msg, dst_ref=got.at[src], send_sem=send.at[d], recv_sem=recv.at[src],
            device_id={"tp": src}, device_id_type=MESH)

    msg1[...] = jnp.zeros_like(msg1)
    for g in range(draft + 1):
        rs = pl.ds(g * batch, batch)
        m = m_ref[rs, :]
        top = jnp.max(m, axis=1, keepdims=True)
        tot = jnp.sum(l_ref[rs, :] * jnp.exp2(m - top), axis=1, keepdims=True)
        msg1[pl.ds(g, 1), pl.ds(0, batch)] = _col_to_row(top + jnp.log2(tot))

    def token_rows(src, dst):
        @pl.loop(0, batch, unroll=8)
        def _(b):
            for j in range(draft):
                idx = tok_smem[j, b] - me * vocab
                idx = jnp.minimum(jnp.maximum(idx, 0), vocab - 1)
                c = lax.shift_right_logical(idx, 7)
                dst[pl.ds(j * batch + b, 1), :] = src[c, pl.ds(b * draft + j, 1), :]

    pl.semaphore_wait(barrier, ntp - 1)
    order = sorted(range(1, ntp), key=lambda d: abs(d - ntp // 2))
    for d in order:
        remote(msg1, got1, send1, recv1, d).start()
    got1[me] = msg1[...]

    @pl.loop(0, q_first)
    def _(c):
        q_copy(c).start()

    for copy in tok_copies:
        copy.wait()
    token_rows(s_ref, gs_buf)
    msg2[...] = jnp.zeros_like(msg2)
    lane = lax.broadcasted_iota(jnp.int32, (batch, LANES), 1)
    for j in range(draft):
        idx = _row_to_col(tok_ref[pl.ds(j, 1), :].astype(jnp.float32)).astype(jnp.int32) - me * vocab
        owned = jnp.logical_and(idx >= 0, idx < vocab)
        hit = jnp.logical_and(owned, lane == jnp.bitwise_and(idx, LANES - 1))
        rs = pl.ds(j * batch, batch)
        tok_s = jnp.sum(jnp.where(hit, gs_buf[rs, :], 0.0), axis=1, keepdims=True)
        q_row = jnp.where(
            lax.shift_right_logical(idx, 7) == nc - 1,
            q_ref[nc - 1, pl.ds(j, batch, stride=draft), :],
            tile_ref[pl.ds((draft + 1) * j, batch, stride=draft * draft), :])
        tok_q = jnp.sum(jnp.where(hit, q_row, 0.0), axis=1, keepdims=True)
        msg2[pl.ds(draft + j, 1), pl.ds(0, batch)] = _col_to_row(tok_s)
        msg2[pl.ds(2 * draft + j, 1), pl.ds(0, batch)] = _col_to_row(tok_q)

    bulk = q_ref.at[pl.ds(0, q_first)]
    pltpu.make_async_copy(bulk, bulk, q_sem).wait()

    for d in range(1, ntp):
        arrived(msg1, got1, send1, recv1, d).wait_recv()
    top = got1[0]
    for i in range(1, ntp):
        top = jnp.maximum(top, got1[i])
    tot = jnp.exp2(got1[0] - top)
    for i in range(1, ntp):
        tot = tot + jnp.exp2(got1[i] - top)
    lse2 = top + jnp.log2(tot)
    bonus_ref[...] = lse2[draft:draft + 1, 0:batch] * LN2
    for j in range(draft):
        col_buf[pl.ds(j, batch, stride=draft), :] = jnp.broadcast_to(
            _row_to_col(lse2[j:j + 1, 0:batch]), (batch, LANES))

    last_mask = lax.broadcasted_iota(jnp.int32, (SLAB, LANES), 1) < last

    @pl.loop(0, batch * draft // SLAB)
    def _(v):
        rs = pl.ds(pl.multiple_of(v * SLAB, SLAB), SLAB)
        lse = col_buf[rs, :]

        def ex(c):
            return jnp.maximum(jnp.exp2(s_ref[c, rs, :] - lse) - q_ref[c, rs, :], 0.0)

        def chunk(t, total):
            for i in range(CHUNK):
                total = total + ex(t * CHUNK + i)
            return total

        part_buf[rs, :] = lax.fori_loop(
            0, (nc - 1) // CHUNK, chunk, jnp.where(last_mask, ex(nc - 1), 0.0))

    for h in range(batch * draft // LANES):
        msg2[pl.ds(h, 1), :] = jnp.sum(part_buf[pl.ds(h * LANES, LANES), :].T, axis=0, keepdims=True)

    for d in order:
        remote(msg2, got2, send2, recv2, d).start()
    got2[me] = msg2[...]
    for d in range(1, ntp):
        arrived(msg2, got2, send2, recv2, d).wait_recv()
    tot = got2[0]
    for i in range(1, ntp):
        tot = tot + got2[i]
    norm_ref[...] = tot[0:draft, :]
    inv = 1.0 / tot[0:draft, :]
    for h in range(batch * draft // LANES):
        inv_ref[pl.ds(h * LANES, LANES), :] = jnp.broadcast_to(inv[h:h + 1, :], (LANES, LANES)).T
    target = jnp.exp2(tot[draft:2 * draft, 0:batch] - lse2[0:draft, 0:batch])
    accept_ref[...] = jnp.minimum(1.0, target / tot[2 * draft:3 * draft, 0:batch])
    for d in range(1, ntp):
        remote(msg1, got1, send1, recv1, d).wait_send()
        remote(msg2, got2, send2, recv2, d).wait_send()


OUT_GROUP = 5


def _write_kernel(
    dims, s_ref, q_ref, lse_ref, inv_ref, accept_in, norm_in, bonus_in,
    out_hbm, accept_ref, norm_ref, bonus_ref, stage, stage_last, norm_col, norm_out, sem,
):
    batch, draft, vocab = dims
    nc = -(-vocab // LANES)
    last = vocab - (nc - 1) * LANES
    view = stage.reshape(nc, batch, draft, LANES)
    ngroups = (nc - 1) // OUT_GROUP
    assert ngroups * OUT_GROUP == nc - 1

    def out_copy(c):
        return pltpu.make_async_copy(
            view.at[c], out_hbm.at[:, :, pl.ds(pl.multiple_of(c * LANES, LANES), LANES)], sem.at[0])

    def fill(c):
        stage[c] = jnp.maximum(jnp.exp2(s_ref[c] - lse_ref[...]) - q_ref[c], 0.0) * inv_ref[...]

    small = [
        pltpu.make_async_copy(src, dst, sem.at[2 + i])
        for i, (src, dst) in enumerate([(accept_in, accept_ref), (norm_out, norm_ref), (bonus_in, bonus_ref)])
    ]
    fill(nc - 1)
    for b in range(batch):
        stage_last[b] = stage[nc - 1, pl.ds(b * draft, draft), pl.ds(0, last)]
    last_copy = pltpu.make_async_copy(stage_last, out_hbm.at[:, :, pl.ds((nc - 1) * LANES, last)], sem.at[1])
    last_copy.start()

    @pl.loop(0, ngroups)
    def _(t):
        for i in range(OUT_GROUP):
            fill(t * OUT_GROUP + i)
            out_copy(t * OUT_GROUP + i).start()

    for h in range(batch * draft // LANES):
        norm_col[pl.ds(h * LANES, LANES), :] = jnp.broadcast_to(norm_in[pl.ds(h, 1), :], (LANES, LANES)).T
    for j in range(draft):
        norm_out[pl.ds(j, 1), :] = _col_to_row(norm_col[pl.ds(j, batch, stride=draft), pl.ds(0, 1)])
    last_copy.wait()
    for copy in small:
        copy.start()
    for copy in small:
        copy.wait()
    bulk = stage.at[pl.ds(0, nc - 1)]
    pltpu.make_async_copy(bulk, bulk, sem.at[0]).wait()


def solution(mesh):
    ntp = mesh.shape["tp"]

    def local_step(hidden, norm_gain, w_head, draft_probs, draft_tokens, temperature):
        batch, draft, vocab = draft_probs.shape
        depth = hidden.shape[2]
        rows = batch * (draft + 1)
        nc = -(-vocab // LANES)
        vmem = pl.BlockSpec(memory_space=pltpu.VMEM)
        hbm = pl.BlockSpec(memory_space=pl.ANY)
        keep = functools.partial(pltpu.with_memory_space_constraint, memory_space=pltpu.VMEM)
        f32, bf16, dma = jnp.float32, jnp.bfloat16, pltpu.SemaphoreType.DMA
        vec = pltpu.VMEM((batch * draft, LANES), f32)
        big = pltpu.VMEM((nc, batch * draft, LANES), f32)
        stat = pltpu.VMEM((rows, LANES), f32)
        x = hidden.transpose(1, 0, 2).reshape(rows, depth)
        tok = draft_tokens.T
        s, q, m, l, tiles = pl.pallas_call(
            functools.partial(_logits_kernel, (batch, draft, depth, vocab)),
            out_shape=(big, big, stat, stat, pltpu.VMEM((batch * draft * draft, LANES), f32)),
            in_specs=[hbm] * 6,
            out_specs=(vmem,) * 5,
            scratch_shapes=[
                pltpu.VMEM((rows, depth), bf16),
                pltpu.VMEM((rows, depth), bf16),
                pltpu.VMEM((RING, STEP, depth), bf16),
                pltpu.VMEM((batch, draft, vocab - (nc - 1) * LANES), f32),
                pltpu.VMEM((batch, LANES), f32),
                pltpu.VMEM((1, depth), f32),
                pltpu.VMEM((1, batch), f32),
                pltpu.SMEM((draft, batch), jnp.int32),
                dma,
                dma((RING, W_PARTS)),
                dma((3,)),
                dma((3,)),
                pltpu.SemaphoreType.REGULAR,
            ],
            compiler_params=pltpu.CompilerParams(vmem_limit_bytes=GRANT),
            name="logits",
        )(x, norm_gain.reshape(1, depth), w_head.T, draft_probs, temperature.reshape(1, batch), tok)
        q, lse, inv, accept, norm, bonus = pl.pallas_call(
            functools.partial(_verify_kernel, (batch, draft, vocab, ntp)),
            out_shape=(
                big,
                vec,
                vec,
                pltpu.VMEM((draft, batch), f32),
                pltpu.VMEM((draft, LANES), f32),
                pltpu.VMEM((1, batch), f32),
            ),
            in_specs=[vmem, vmem, vmem, vmem, vmem, hbm, hbm],
            out_specs=(vmem,) * 6,
            input_output_aliases={1: 0},
            scratch_shapes=[
                vec, vec,
                pltpu.SMEM((draft, batch), jnp.int32),
                pltpu.VMEM((draft, batch), jnp.int32),
                pltpu.VMEM((8, LANES), f32),
                pltpu.VMEM((16, LANES), f32),
                pltpu.VMEM((ntp, 8, LANES), f32),
                pltpu.VMEM((ntp, 16, LANES), f32),
                dma((ntp,)), dma((ntp,)), dma((ntp,)), dma((ntp,)), dma, dma((2,)),
            ],
            compiler_params=pltpu.CompilerParams(
                collective_id=0, has_side_effects=True, vmem_limit_bytes=GRANT),
            name="verify",
        )(keep(s), keep(q), keep(m), keep(l), keep(tiles), tok, draft_probs)
        residual, accept, norm, bonus = pl.pallas_call(
            functools.partial(_write_kernel, (batch, draft, vocab)),
            out_shape=(
                jax.ShapeDtypeStruct(draft_probs.shape, f32),
                jax.ShapeDtypeStruct((draft, batch), f32),
                jax.ShapeDtypeStruct((draft, batch), f32),
                jax.ShapeDtypeStruct((1, batch), f32),
            ),
            in_specs=[vmem] * 7,
            out_specs=(hbm,) * 4,
            scratch_shapes=[
                big,
                pltpu.VMEM((batch, draft, vocab - (nc - 1) * LANES), f32),
                vec,
                pltpu.VMEM((draft, batch), f32),
                dma((5,)),
            ],
            compiler_params=pltpu.CompilerParams(vmem_limit_bytes=GRANT),
            name="write",
        )(*map(keep, (s, q, lse, inv, accept, norm, bonus)))
        return accept.T, norm.T, residual, bonus.reshape(batch)

    return jax.shard_map(
        local_step,
        mesh=mesh,
        in_specs=(P('dp', None, None), P(), P(None, 'tp'), P('dp', None, 'tp'), P('dp', None), P('dp')),
        out_specs=(P('dp', None), P('dp', None), P('dp', None, 'tp'), P('dp')),
        check_vma=False,
    )
```

```python
import functools

import jax
import jax.numpy as jnp
from jax import lax
from jax.experimental import pallas as pl
from jax.experimental.pallas import tpu as pltpu
from jax.sharding import PartitionSpec as P

LANES = 128
TILE = 256
STEP = 2 * TILE
RING = 10
SLAB = 64
CHUNK = 25
W_PARTS = 2
FENCES = 6
Q_LATE = 3
TOK_STEP = 8
SIG = (1, 3, 5, 7)
GRP = {1: (0,), 3: (1, 2), 5: (3, 4)}
GRANT = 26 * 1024 * 1024
LOG2E = 1.4426950408889634
LN2 = 0.6931471805599453
LOWEST = -3.4028234e38
MESH = pl.DeviceIdType.MESH


def _row_to_col(row):
    n = row.shape[1]
    r = lax.broadcasted_iota(jnp.int32, (n, n), 0)
    c = lax.broadcasted_iota(jnp.int32, (n, n), 1)
    return jnp.sum(jnp.where(r == c, row, 0.0), axis=1, keepdims=True)


def _col_to_row(col):
    n = col.shape[0]
    r = lax.broadcasted_iota(jnp.int32, (n, n), 0)
    c = lax.broadcasted_iota(jnp.int32, (n, n), 1)
    return jnp.sum(jnp.where(r == c, col, 0.0), axis=0, keepdims=True)


def _q_first(vocab):
    return (vocab // LANES) * Q_LATE // 8


def _logits_kernel(
    dims,
    x_hbm, gain_hbm, w_hbm, q_hbm, temp_hbm, tok_hbm,
    s_ref, q_buf, m_buf, l_buf, tile_ref,
    h_buf, x_buf, w_buf, q_last, scale_buf, gain_ref, temp_ref, tok_smem,
    h_sem, w_sem, q_sem, small_sem, fence,
):
    batch, draft, depth, vocab = dims
    tokens = batch * draft
    me = lax.axis_index("tp")
    q_first = _q_first(vocab)
    rows = batch * (draft + 1)
    nk = depth // TILE
    full = vocab // STEP
    rest = vocab - full * STEP
    nc = -(-vocab // LANES)
    last = vocab - (nc - 1) * LANES
    part = STEP // W_PARTS

    def w_copy(n, i, size=part):
        slot = lax.rem(n, RING)
        return pltpu.make_async_copy(
            w_hbm.at[pl.ds(n * STEP + i * part, size), :], w_buf.at[slot, pl.ds(i * part, size), :], w_sem.at[slot])

    def w_wait(n):
        for i in range(W_PARTS):
            w_copy(n, i).wait()

    def w_rest():
        return [w_copy(full, i, min(part, rest - i * part)) for i in range(-(-rest // part))]

    tiles = tile_ref.reshape(tokens, draft, LANES)
    qv = q_buf.reshape(nc, batch, draft, LANES)

    def q_copy(c):
        return pltpu.make_async_copy(
            q_hbm.at[:, :, pl.ds(pl.multiple_of(c * LANES, LANES), LANES)], qv.at[c], q_sem.at[0])

    def token_copy(b, j):
        idx = tok_smem[j, b] - me * vocab
        c = lax.shift_right_logical(jnp.minimum(jnp.maximum(idx, 0), vocab - 1), 7)
        c = jnp.minimum(c, nc - 2)
        return pltpu.make_async_copy(
            q_hbm.at[b, :, pl.ds(pl.multiple_of(c * LANES, LANES), LANES)], tiles.at[b * draft + j], q_sem.at[2])

    def last_q():
        return pltpu.make_async_copy(
            q_hbm.at[:, :, pl.ds((nc - 1) * LANES, last)], q_last, q_sem.at[1])

    def h_copy(g):
        rs = pl.ds(g * batch, batch)
        return pltpu.make_async_copy(x_hbm.at[rs, :], h_buf.at[rs, :], h_sem)

    small = [
        pltpu.make_async_copy(src, dst, small_sem.at[i])
        for i, (src, dst) in enumerate([(gain_hbm, gain_ref), (temp_hbm, temp_ref), (tok_hbm, tok_smem)])
    ]
    for g in range(draft + 1):
        h_copy(g).start()
    for copy in small:
        copy.start()
    for n in range(RING - 1):
        for i in range(W_PARTS):
            w_copy(n, i).start(priority=i % 2)
    last_q().start(priority=1)

    m_buf[...] = jnp.full_like(m_buf, LOWEST)
    l_buf[...] = jnp.zeros_like(l_buf)

    groups = draft + 1

    def online(g, q, c0, z, ncol, penalty=None):
        rs = pl.ds(g * batch, batch)
        scale = scale_buf[...]
        ss = [z[:, i * LANES:(i + 1) * LANES] * scale for i in range(ncol)]
        if penalty is not None:
            ss = [s + p for s, p in zip(ss, penalty)]
        m_old = m_buf[rs, :]
        m_new = m_old
        for s in ss:
            m_new = jnp.maximum(m_new, s)
        l = l_buf[rs, :] * jnp.exp2(m_old - m_new)
        for s in ss:
            l = l + jnp.exp2(s - m_new)
        m_buf[rs, :] = m_new
        l_buf[rs, :] = l
        if g < draft:
            for i in range(ncol):
                s_ref[c0 + i, pl.ds(g, batch, stride=draft), :] = ss[i]

    def lhs(g, k):
        return x_buf[pl.ds(g * batch, batch), pl.ds(k * TILE, TILE)]

    def push(n, q, k):
        slot = lax.rem(n, RING)
        w = w_buf[slot, pl.ds(q * TILE, TILE), pl.ds(k * TILE, TILE)]
        pltpu.matmul_push_rhs(w, staging_register=k % 2, mxu_index=q, transpose=True)

    def mxu_body(*accs):
        acc = [[[accs[(a * 2 + q) * groups + g] for g in range(groups)] for q in range(2)] for a in range(2)]
        for a in range(2):
            for q in range(2):
                for g in range(groups):
                    pltpu.matmul_pop(acc[a][q][g])

        for copy in small:
            copy.wait()
        scale_buf[...] = jnp.broadcast_to(LOG2E / _row_to_col(temp_ref[...]), (batch, LANES))
        for g in range(draft + 1):
            h_copy(g).wait()
        for i in range(rows // 32):
            sl = pl.ds(i * 32, 32)
            h = h_buf[sl, :].astype(jnp.float32)
            r = lax.rsqrt(jnp.mean(h * h, axis=-1, keepdims=True) + 1e-5)
            x_buf[sl, :] = (h_buf[sl, :].astype(jnp.float32) * r * gain_ref[...]).astype(jnp.bfloat16)

        half = nk // 2

        def push_rest(q, kk):
            w = w_buf[full % RING, pl.ds(0, TILE), pl.ds((q * half + kk) * TILE, TILE)]
            pltpu.matmul_push_rhs(w, staging_register=kk % 2, mxu_index=q, transpose=True)

        def fullstep(n, a, issue, penalty=None, next_full=True):
            old = acc[1 - a]
            c_old = jnp.maximum(n - 1, 0) * (STEP // LANES)
            for k in range(nk):
                for q in range(2):
                    for g in range(groups):
                        pltpu.matmul_acc_lhs(acc[a][q][g], lhs(g, k), load_staged_rhs=k % 2 if g == 0 else None)
                for q in range(2):
                    if k + 1 < nk:
                        push(n, q, k + 1)
                    elif next_full:
                        push(n + 1, q, 0)
                    else:
                        push_rest(q, 0)
                if 1 <= k <= FENCES:
                    issue(k - 1)
                if k in SIG:
                    pl.semaphore_signal(fence, 1)
                for g in GRP.get(k, ()):
                    for q in range(2):
                        z = pltpu.matmul_pop(old[q][g])
                        online(g, q, c_old + q * (TILE // LANES), z, TILE // LANES,
                               None if penalty is None else [penalty] * (TILE // LANES))


        w_wait(0)
        for q in range(2):
            push(0, q, 0)

        split = (full - (RING - 1)) // 2 * 2
        tail = full // 2 * 2
        early = 1
        mid = nc - 1 - q_first - early * split
        assert mid >= 0 and tail == full - 1 and tokens >= TOK_STEP * full

        def issue_tokens(n):
            for i in range(TOK_STEP):
                token_copy(n * (TOK_STEP // draft) + i // draft, i % draft).start(priority=1)

        def issue_early(n, i):
            if i < W_PARTS:
                w_copy(n + RING - 1, i).start(priority=i % 2)
            elif i == W_PARTS:
                q_copy(q_first + n).start(priority=1)
            elif i == W_PARTS + 1:
                issue_tokens(n)

        def issue_late(n, i):
            if i == W_PARTS + 1:
                issue_tokens(n)

        @pl.loop(0, split // 2)
        def _(t):
            n = 2 * t
            w_wait(n + 1)
            fullstep(n, 0, lambda i: issue_early(n, i), penalty=jnp.where(t == 0, LOWEST, 0.0).astype(jnp.float32))
            w_wait(n + 2)
            fullstep(n + 1, 1, lambda i: issue_early(n + 1, i))

        for i, copy in enumerate(w_rest()):
            copy.start(priority=i % 2)

        @pl.loop(0, mid)
        def _(i):
            q_copy(q_first + early * split + i).start(priority=1)

        for i in range(TOK_STEP * full, tokens):
            token_copy(i // draft, i % draft).start(priority=1)

        @pl.loop(split // 2, tail // 2)
        def _(t):
            n = 2 * t
            w_wait(n + 1)
            fullstep(n, 0, lambda i: issue_late(n, i))
            w_wait(n + 2)
            fullstep(n + 1, 1, lambda i: issue_late(n + 1, i))

        n = full - 1
        for copy in w_rest():
            copy.wait()
        last_q().wait()
        for b in range(0, batch, 2):
            q_buf[nc - 1, pl.ds(b * draft, 2 * draft), pl.ds(0, last)] = jnp.concatenate([q_last[b], q_last[b + 1]], axis=0)
        fullstep(n, 0, lambda i: issue_late(n, i), next_full=False)
        pl.semaphore_wait(fence, len(SIG) * full)
        for kk in range(half):
            for q in range(2):
                for g in range(groups):
                    pltpu.matmul_acc_lhs(acc[1][q][g], lhs(g, q * half + kk), load_staged_rhs=kk % 2 if g == 0 else None)
                if kk + 1 < half:
                    push_rest(q, kk + 1)
        for g in range(groups):
            for q in range(2):
                z = pltpu.matmul_pop(acc[0][q][g])
                online(g, q, n * (STEP // LANES) + q * (TILE // LANES), z, TILE // LANES)
        ncol = -(-rest // LANES)
        lane = lax.broadcasted_iota(jnp.int32, (batch, LANES), 1)
        pens = [None] * ncol
        for i in range(ncol):
            pens[i] = jnp.where(lane + i * LANES < rest, 0.0, LOWEST)
        for g in range(groups):
            z = pltpu.matmul_pop(acc[1][0][g]) + pltpu.matmul_pop(acc[1][1][g])
            online(g, 0, full * (STEP // LANES), z, ncol, pens)

    specs = [pltpu.ACC(q)((batch, TILE), jnp.float32) for a in range(2) for q in range(2) for g in range(groups)]
    pl.run_scoped(mxu_body, *specs)

    bulk = q_buf.at[pl.ds(q_first, nc - 1 - q_first)]
    pltpu.make_async_copy(bulk, bulk, q_sem.at[0]).wait()
    pltpu.make_async_copy(tile_ref, tile_ref, q_sem.at[2]).wait()


def _verify_kernel(
    dims,
    s_ref, q_in, m_ref, l_ref, tile_ref, tok_hbm, q_hbm,
    q_ref, col_buf, inv_ref, accept_ref, norm_ref, bonus_ref,
    gs_buf, part_buf, tok_smem, tok_ref,
    msg1, msg2, got1, got2,
    send1, recv1, send2, recv2, q_sem, tok_sem,
):
    del q_in
    batch, draft, vocab, ntp = dims
    nc = -(-vocab // LANES)
    last = vocab - (nc - 1) * LANES
    me = lax.axis_index("tp")
    barrier = pltpu.get_barrier_semaphore()
    for d in range(1, ntp):
        pl.semaphore_signal(barrier, inc=1, device_id={"tp": lax.rem(me + d, ntp)}, device_id_type=MESH)
    q_first = _q_first(vocab)
    qv = q_ref.reshape(nc, batch, draft, LANES)

    def q_copy(c):
        return pltpu.make_async_copy(
            q_hbm.at[:, :, pl.ds(pl.multiple_of(c * LANES, LANES), LANES)], qv.at[c], q_sem)

    tok_copies = [
        pltpu.make_async_copy(tok_hbm, tok_smem, tok_sem.at[0]),
        pltpu.make_async_copy(tok_hbm, tok_ref, tok_sem.at[1]),
    ]
    for copy in tok_copies:
        copy.start()

    def remote(msg, got, send, recv, d):
        return pltpu.make_async_remote_copy(
            src_ref=msg, dst_ref=got.at[me], send_sem=send.at[d], recv_sem=recv.at[me],
            device_id={"tp": lax.rem(me + d, ntp)}, device_id_type=MESH)

    def arrived(msg, got, send, recv, d):
        src = lax.rem(me + d, ntp)
        return pltpu.make_async_remote_copy(
            src_ref=msg, dst_ref=got.at[src], send_sem=send.at[d], recv_sem=recv.at[src],
            device_id={"tp": src}, device_id_type=MESH)

    msg1[...] = jnp.zeros_like(msg1)
    for g in range(draft + 1):
        rs = pl.ds(g * batch, batch)
        m = m_ref[rs, :]
        top = jnp.max(m, axis=1, keepdims=True)
        tot = jnp.sum(l_ref[rs, :] * jnp.exp2(m - top), axis=1, keepdims=True)
        msg1[pl.ds(g, 1), pl.ds(0, batch)] = _col_to_row(top + jnp.log2(tot))

    def token_rows(src, dst):
        @pl.loop(0, batch, unroll=8)
        def _(b):
            for j in range(draft):
                idx = tok_smem[j, b] - me * vocab
                idx = jnp.minimum(jnp.maximum(idx, 0), vocab - 1)
                c = lax.shift_right_logical(idx, 7)
                dst[pl.ds(j * batch + b, 1), :] = src[c, pl.ds(b * draft + j, 1), :]

    pl.semaphore_wait(barrier, ntp - 1)
    order = sorted(range(1, ntp), key=lambda d: abs(d - ntp // 2))
    for d in order:
        remote(msg1, got1, send1, recv1, d).start()
    got1[me] = msg1[...]

    @pl.loop(0, q_first)
    def _(c):
        q_copy(c).start()

    for copy in tok_copies:
        copy.wait()
    token_rows(s_ref, gs_buf)
    msg2[...] = jnp.zeros_like(msg2)
    lane = lax.broadcasted_iota(jnp.int32, (batch, LANES), 1)
    for j in range(draft):
        idx = _row_to_col(tok_ref[pl.ds(j, 1), :].astype(jnp.float32)).astype(jnp.int32) - me * vocab
        owned = jnp.logical_and(idx >= 0, idx < vocab)
        hit = jnp.logical_and(owned, lane == jnp.bitwise_and(idx, LANES - 1))
        rs = pl.ds(j * batch, batch)
        tok_s = jnp.sum(jnp.where(hit, gs_buf[rs, :], 0.0), axis=1, keepdims=True)
        q_row = jnp.where(
            lax.shift_right_logical(idx, 7) == nc - 1,
            q_ref[nc - 1, pl.ds(j, batch, stride=draft), :],
            tile_ref[pl.ds((draft + 1) * j, batch, stride=draft * draft), :])
        tok_q = jnp.sum(jnp.where(hit, q_row, 0.0), axis=1, keepdims=True)
        msg2[pl.ds(draft + j, 1), pl.ds(0, batch)] = _col_to_row(tok_s)
        msg2[pl.ds(2 * draft + j, 1), pl.ds(0, batch)] = _col_to_row(tok_q)

    bulk = q_ref.at[pl.ds(0, q_first)]
    pltpu.make_async_copy(bulk, bulk, q_sem).wait()

    for d in range(1, ntp):
        arrived(msg1, got1, send1, recv1, d).wait_recv()
    top = got1[0]
    for i in range(1, ntp):
        top = jnp.maximum(top, got1[i])
    tot = jnp.exp2(got1[0] - top)
    for i in range(1, ntp):
        tot = tot + jnp.exp2(got1[i] - top)
    lse2 = top + jnp.log2(tot)
    bonus_ref[...] = lse2[draft:draft + 1, 0:batch] * LN2
    for j in range(draft):
        col_buf[pl.ds(j, batch, stride=draft), :] = jnp.broadcast_to(
            _row_to_col(lse2[j:j + 1, 0:batch]), (batch, LANES))

    last_mask = lax.broadcasted_iota(jnp.int32, (SLAB, LANES), 1) < last

    @pl.loop(0, batch * draft // SLAB)
    def _(v):
        rs = pl.ds(pl.multiple_of(v * SLAB, SLAB), SLAB)
        lse = col_buf[rs, :]

        def ex(c):
            return jnp.maximum(jnp.exp2(s_ref[c, rs, :] - lse) - q_ref[c, rs, :], 0.0)

        def chunk(t, total):
            for i in range(CHUNK):
                total = total + ex(t * CHUNK + i)
            return total

        part_buf[rs, :] = lax.fori_loop(
            0, (nc - 1) // CHUNK, chunk, jnp.where(last_mask, ex(nc - 1), 0.0))

    for h in range(batch * draft // LANES):
        msg2[pl.ds(h, 1), :] = jnp.sum(part_buf[pl.ds(h * LANES, LANES), :].T, axis=0, keepdims=True)

    for d in order:
        remote(msg2, got2, send2, recv2, d).start()
    got2[me] = msg2[...]
    for d in range(1, ntp):
        arrived(msg2, got2, send2, recv2, d).wait_recv()
    tot = got2[0]
    for i in range(1, ntp):
        tot = tot + got2[i]
    norm_ref[...] = tot[0:draft, :]
    inv = 1.0 / tot[0:draft, :]
    for h in range(batch * draft // LANES):
        inv_ref[pl.ds(h * LANES, LANES), :] = jnp.broadcast_to(inv[h:h + 1, :], (LANES, LANES)).T
    target = jnp.exp2(tot[draft:2 * draft, 0:batch] - lse2[0:draft, 0:batch])
    accept_ref[...] = jnp.minimum(1.0, target / tot[2 * draft:3 * draft, 0:batch])
    for d in range(1, ntp):
        remote(msg1, got1, send1, recv1, d).wait_send()
        remote(msg2, got2, send2, recv2, d).wait_send()


OUT_GROUP = 5


def _write_kernel(
    dims, s_ref, q_ref, lse_ref, inv_ref, accept_in, norm_in, bonus_in,
    out_hbm, accept_ref, norm_ref, bonus_ref, stage, stage_last, norm_col, norm_out, sem,
):
    batch, draft, vocab = dims
    nc = -(-vocab // LANES)
    last = vocab - (nc - 1) * LANES
    view = stage.reshape(nc, batch, draft, LANES)
    ngroups = (nc - 1) // OUT_GROUP
    assert ngroups * OUT_GROUP == nc - 1

    def out_copy(c):
        return pltpu.make_async_copy(
            view.at[c], out_hbm.at[:, :, pl.ds(pl.multiple_of(c * LANES, LANES), LANES)], sem.at[0])

    def fill(c):
        stage[c] = jnp.maximum(jnp.exp2(s_ref[c] - lse_ref[...]) - q_ref[c], 0.0) * inv_ref[...]

    small = [
        pltpu.make_async_copy(src, dst, sem.at[2 + i])
        for i, (src, dst) in enumerate([(accept_in, accept_ref), (norm_out, norm_ref), (bonus_in, bonus_ref)])
    ]
    fill(nc - 1)
    for b in range(batch):
        stage_last[b] = stage[nc - 1, pl.ds(b * draft, draft), pl.ds(0, last)]
    last_copy = pltpu.make_async_copy(stage_last, out_hbm.at[:, :, pl.ds((nc - 1) * LANES, last)], sem.at[1])
    last_copy.start()

    @pl.loop(0, ngroups)
    def _(t):
        for i in range(OUT_GROUP):
            fill(t * OUT_GROUP + i)
            out_copy(t * OUT_GROUP + i).start()

    for h in range(batch * draft // LANES):
        norm_col[pl.ds(h * LANES, LANES), :] = jnp.broadcast_to(norm_in[pl.ds(h, 1), :], (LANES, LANES)).T
    for j in range(draft):
        norm_out[pl.ds(j, 1), :] = _col_to_row(norm_col[pl.ds(j, batch, stride=draft), pl.ds(0, 1)])
    last_copy.wait()
    for copy in small:
        copy.start()
    for copy in small:
        copy.wait()
    bulk = stage.at[pl.ds(0, nc - 1)]
    pltpu.make_async_copy(bulk, bulk, sem.at[0]).wait()


def solution(mesh):
    ntp = mesh.shape["tp"]

    def local_step(hidden, norm_gain, w_head, draft_probs, draft_tokens, temperature):
        batch, draft, vocab = draft_probs.shape
        depth = hidden.shape[2]
        rows = batch * (draft + 1)
        nc = -(-vocab // LANES)
        vmem = pl.BlockSpec(memory_space=pltpu.VMEM)
        hbm = pl.BlockSpec(memory_space=pl.ANY)
        keep = functools.partial(pltpu.with_memory_space_constraint, memory_space=pltpu.VMEM)
        f32, bf16, dma = jnp.float32, jnp.bfloat16, pltpu.SemaphoreType.DMA
        vec = pltpu.VMEM((batch * draft, LANES), f32)
        big = pltpu.VMEM((nc, batch * draft, LANES), f32)
        stat = pltpu.VMEM((rows, LANES), f32)
        x = hidden.transpose(1, 0, 2).reshape(rows, depth)
        tok = draft_tokens.T
        s, q, m, l, tiles = pl.pallas_call(
            functools.partial(_logits_kernel, (batch, draft, depth, vocab)),
            out_shape=(big, big, stat, stat, pltpu.VMEM((batch * draft * draft, LANES), f32)),
            in_specs=[hbm] * 6,
            out_specs=(vmem,) * 5,
            scratch_shapes=[
                pltpu.VMEM((rows, depth), bf16),
                pltpu.VMEM((rows, depth), bf16),
                pltpu.VMEM((RING, STEP, depth), bf16),
                pltpu.VMEM((batch, draft, vocab - (nc - 1) * LANES), f32),
                pltpu.VMEM((batch, LANES), f32),
                pltpu.VMEM((1, depth), f32),
                pltpu.VMEM((1, batch), f32),
                pltpu.SMEM((draft, batch), jnp.int32),
                dma,
                dma((RING,)),
                dma((3,)),
                dma((3,)),
                pltpu.SemaphoreType.REGULAR,
            ],
            compiler_params=pltpu.CompilerParams(vmem_limit_bytes=GRANT),
            name="logits",
        )(x, norm_gain.reshape(1, depth), w_head.T, draft_probs, temperature.reshape(1, batch), tok)
        q, lse, inv, accept, norm, bonus = pl.pallas_call(
            functools.partial(_verify_kernel, (batch, draft, vocab, ntp)),
            out_shape=(
                big,
                vec,
                vec,
                pltpu.VMEM((draft, batch), f32),
                pltpu.VMEM((draft, LANES), f32),
                pltpu.VMEM((1, batch), f32),
            ),
            in_specs=[vmem, vmem, vmem, vmem, vmem, hbm, hbm],
            out_specs=(vmem,) * 6,
            input_output_aliases={1: 0},
            scratch_shapes=[
                vec, vec,
                pltpu.SMEM((draft, batch), jnp.int32),
                pltpu.VMEM((draft, batch), jnp.int32),
                pltpu.VMEM((8, LANES), f32),
                pltpu.VMEM((16, LANES), f32),
                pltpu.VMEM((ntp, 8, LANES), f32),
                pltpu.VMEM((ntp, 16, LANES), f32),
                dma((ntp,)), dma((ntp,)), dma((ntp,)), dma((ntp,)), dma, dma((2,)),
            ],
            compiler_params=pltpu.CompilerParams(
                collective_id=0, has_side_effects=True, vmem_limit_bytes=GRANT),
            name="verify",
        )(keep(s), keep(q), keep(m), keep(l), keep(tiles), tok, draft_probs)
        residual, accept, norm, bonus = pl.pallas_call(
            functools.partial(_write_kernel, (batch, draft, vocab)),
            out_shape=(
                jax.ShapeDtypeStruct(draft_probs.shape, f32),
                jax.ShapeDtypeStruct((draft, batch), f32),
                jax.ShapeDtypeStruct((draft, batch), f32),
                jax.ShapeDtypeStruct((1, batch), f32),
            ),
            in_specs=[vmem] * 7,
            out_specs=(hbm,) * 4,
            scratch_shapes=[
                big,
                pltpu.VMEM((batch, draft, vocab - (nc - 1) * LANES), f32),
                vec,
                pltpu.VMEM((draft, batch), f32),
                dma((5,)),
            ],
            compiler_params=pltpu.CompilerParams(vmem_limit_bytes=GRANT),
            name="write",
        )(*map(keep, (s, q, lse, inv, accept, norm, bonus)))
        return accept.T, norm.T, residual, bonus.reshape(batch)

    return jax.shard_map(
        local_step,
        mesh=mesh,
        in_specs=(P('dp', None, None), P(), P(None, 'tp'), P('dp', None, 'tp'), P('dp', None), P('dp')),
        out_specs=(P('dp', None), P('dp', None), P('dp', None, 'tp'), P('dp')),
        check_vma=False,
    )
```
